768 devices in a mesh: gx: 48 (over x_hi, z, core), gy: 16 (over x_lo, y).
Axes of the slice: x: 4 (x_hi: 2, x_lo: 2; x = x_hi * 2 + x_lo), y: 8, z: 12, core: 2. Of those that a mesh axis runs over, the one named last changes fastest.
Arguments:
- velocity: float32 [3, 768, 256, 128], P(None, 'gx', 'gy'), may hold values from -6 to 6
- stresses: float32 [6, 768, 256, 128], P(None, 'gx', 'gy'), may hold values from -6 to 6
- buoyancy: float32 [768, 256, 128], P('gx', 'gy'), may hold values from 0.3 to 0.6
- lame_first: float32 [768, 256, 128], P('gx', 'gy'), may hold values from 0.05 to 0.15
- rigidity: float32 [768, 256, 128], P('gx', 'gy'), may hold values from 0.04 to 0.12
- histories: bfloat16 [196608, 512], P(('gx', 'gy')), may hold values from -6 to 6
- mechanism: bfloat16 [196608, 6], P(('gx', 'gy')), may hold values from -6 to 6
- resample: bfloat16 [512, 3], replicated, may hold values from -0.25 to 0.25
- owners: int32 [196608, 1], P(('gx', 'gy')), may hold values from 0 to 15; in each aligned block of 256 rows (0 to 255, 256 to 511, ...) at most 64 rows name the same one
- cell_offsets: int32 [196608], P(('gx', 'gy')), may hold values from 0 to 32767
Outputs:
- velocity_out: float32 [3, 768, 256, 128], P(None, 'gx', 'gy')
- stresses_out: float32 [6, 768, 256, 128], P(None, 'gx', 'gy')
The draws below stay inside these ranges and needn't reach their ends.
Inputs may be any that keep to these rules, and one draw needn't show every extreme that they name: `owners`: among the 256 rows of one device at most 64 name the same owner, a bound that some block reaches of them. `cell_offsets`: cell index x * 16 * 128 + y * 128 + z within the enclosing block.
All inputs are finite; a program needn't handle non-finite values.
Results may differ from the reference program's by a relative error of at most 0.00052.
Values may be sent and summed in bfloat16 or wider, within the bound.
No kernel may reach another device: no remote copies, remote signals or barrier semaphores. Data moves between devices by JAX's collectives and lax.ppermute only.
A program may use at most 32 MiB of HBM per device.

```python
import math
import jax
import jax.numpy as jnp
import numpy as np
from jax import lax

CX = 16
CY = 16
CZ = 128
STEPS = 3
SAMPLES = 512
SRC_DEV = 256
CAP = 64
NX = 768
NY = 256
SOURCES = 196608
N_GY = 16


def plant(values, stream_key, least, high):
    shape = values.shape
    place = [jax.random.randint(jax.random.fold_in(stream_key, axis), (), 0, shape[axis]) for axis in range(len(shape))]
    values = values.at[tuple(place)].set(least)
    longest = shape.index(max(shape))
    place[longest] = (place[longest] + 1) % shape[longest]
    return values.at[tuple(place)].set(high)


def block_levels(rng, dims, shards, least, high):
    def one(position, blocks):
        heights = jax.random.uniform(jax.random.fold_in(jax.random.fold_in(rng, 6), position), (blocks,), jnp.float32, least / len(shards), high / len(shards))
        return jnp.repeat(jnp.exp(heights), dims[position] // blocks).reshape((-1,) + (1,) * (len(dims) - position - 1))

    gain = one(*shards[0])
    for cut in shards[1:]:
        gain = gain * one(*cut)
    return gain


def routed_block(key, own, number, rows, count, top, bound, skew):
    sequence = jax.random.permutation(key, count)
    packed, ordinary = shares(count, rows * top, bound, skew, True), shares(count, rows * top, bound, skew, False)
    places = jnp.arange(count)

    def named(lengths, turn):
        used = int((lengths > 0).sum())
        fixed = max(1, used // 4)
        moved = fixed + (places - fixed + turn * (used - fixed)) % max(1, count - fixed)
        return jnp.zeros((count,), jnp.int32).at[sequence[jnp.where(places < fixed, places, moved)]].set(jnp.asarray(lengths, jnp.int32))

    lengths = jnp.where(number % 4 == 0, named(packed, number // 4), named(ordinary, number - number // 4 - 1))
    mixed = jax.random.permutation(jax.random.fold_in(own, 3), count)
    donor, taker = mixed[0:count // 2 * 2:2], mixed[1:count // 2 * 2:2]
    margin = jnp.minimum(lengths[donor] - 1, bound - lengths[taker]) // 2
    margin = jnp.where((donor == sequence[0]) | (taker == sequence[0]) | (lengths[taker] == 0), 0, jnp.maximum(margin, 0))
    moved = jax.random.randint(jax.random.fold_in(own, 4), (count // 2,), 0, 1 << 20) % (margin + 1)
    lengths = lengths.at[donor].add(-moved).at[taker].add(moved)
    items = jnp.searchsorted(jnp.cumsum(lengths), jnp.arange(rows * top), side="right").astype(jnp.int32)
    table = items.reshape(top, rows).T
    table = table[jax.random.permutation(jax.random.fold_in(own, 1), rows)]
    turn = jax.random.randint(jax.random.fold_in(own, 2), (rows, 1), 0, top)
    return jnp.take_along_axis(table, (jnp.arange(top)[None, :] + turn) % top, axis=1)


def shares(number_of, total, bound, skew, full):
    portions = [(1 << 20) // math.isqrt(standing ** skew) + 1 for standing in range(1, number_of + 1)]
    largest = bound if full else min(bound, max(-(-total // number_of), total * portions[0] // sum(portions)))
    least = 1 if total - largest >= number_of - 1 else 0
    counts, spare = [largest] + [least] * (number_of - 1), total - largest - least * (number_of - 1)
    while spare > 0:
        movable = [i for i in range(1, number_of) if counts[i] < largest] or [i for i in range(1, number_of) if counts[i] < bound]
        whole, left = sum([portions[i] for i in movable]), spare
        for i in movable:
            extra = min(bound - counts[i], max(1, left * portions[i] // whole), spare)
            counts[i] = counts[i] + extra
            spare = spare - extra
    return np.array(counts)


def noise(stream_key, dims, width, limit, split=(), kind=jnp.bfloat16):
    drawn = jax.random.normal(stream_key, dims, jnp.float32) * width
    if len(split) > 0:
        drawn = block_levels(stream_key, dims, split, -0.22, 0.18) * drawn
    return jnp.clip(drawn, min=-limit, max=limit).astype(kind)


def setup_inputs(seed: int = 0) -> dict:
    arg_keys = jax.random.split(jax.random.key(seed), 11)
    velocity = noise(arg_keys[0], (3, NX, NY, CZ), 1.0, 6.0, ((1, 48), (2, 16)), jnp.float32)
    stresses = noise(arg_keys[1], (6, NX, NY, CZ), 1.0, 6.0, ((1, 48), (2, 16)), jnp.float32)
    buoyancy = jnp.clip(jnp.exp(math.log(0.6) - 0.6931472 * jax.random.uniform(arg_keys[2], (NX, NY, CZ), jnp.float32) ** block_levels(arg_keys[2], (NX, NY, CZ), ((0, 48), (1, 16)), -0.2, 0.2)), 0.3, 0.6)
    lame_first = jnp.clip(0.05 + 0.10000001 * jax.random.uniform(arg_keys[3], (NX, NY, CZ), jnp.float32) ** block_levels(arg_keys[3], (NX, NY, CZ), ((0, 48), (1, 16)), -0.2, 0.2), 0.05, 0.15)
    rigidity = jnp.clip(jnp.exp(math.log(0.12) - 1.0986123 * jax.random.uniform(arg_keys[4], (NX, NY, CZ), jnp.float32) ** block_levels(arg_keys[4], (NX, NY, CZ), ((0, 48), (1, 16)), -0.2, 0.2)), 0.04, 0.12)
    histories = noise(arg_keys[5], (SOURCES, SAMPLES), 1.0, 6.0, ((0, 768),))
    mechanism = noise(arg_keys[6], (SOURCES, 6), 1.0, 6.0, ((0, 768),))
    resample = noise(arg_keys[7], (SAMPLES, STEPS), SAMPLES ** -0.5, 0.25)
    owners_keys = jax.random.split(jax.random.fold_in(arg_keys[8], 1), SOURCES // SRC_DEV)
    owners_turns = jax.random.permutation(jax.random.fold_in(arg_keys[8], 3), SOURCES // SRC_DEV)
    owners = jax.vmap(lambda own, number: routed_block(jax.random.fold_in(arg_keys[8], 2), own, number, SRC_DEV, N_GY, 1, CAP, 2))(owners_keys, owners_turns).reshape((SOURCES, 1))
    cell_offsets = plant(jax.random.randint(arg_keys[9], (SOURCES,), 0, CX * CY * CZ), jax.random.fold_in(arg_keys[9], 1), 0, (CX * CY * CZ) - 1).astype(jnp.int32)
    return {"velocity": velocity, "stresses": stresses, "buoyancy": buoyancy, "lame_first": lame_first, "rigidity": rigidity, "histories": histories, "mechanism": mechanism, "resample": resample, "owners": owners, "cell_offsets": cell_offsets}


INNER_WEIGHT = 9.0 / 8.0
OUTER_WEIGHT = -1.0 / 24.0


def differ(values, dimension, forward):
    if dimension == 2:
        values = jnp.pad(values, ((0, 0), (0, 0), (2, 2)))
    extent = values.shape[dimension] - 4

    def window(start_at):
        return lax.slice_in_dim(values, start_at, start_at + extent, axis=dimension)

    if forward:
        result = INNER_WEIGHT * (window(3) - window(2)) + OUTER_WEIGHT * (window(4) - window(1))
    else:
        result = INNER_WEIGHT * (window(2) - window(1)) + OUTER_WEIGHT * (window(3) - window(0))
    for second in (0, 1):
        if second != dimension:
            result = lax.slice_in_dim(result, 2, result.shape[second] - 2, axis=second)
    return result


def advance_velocity(velocity, stresses, buoyancy):
    forces = jnp.stack([
        differ(stresses[0], 0, True) + differ(stresses[3], 1, False) + differ(stresses[4], 2, False),
        differ(stresses[3], 0, False) + differ(stresses[1], 1, True) + differ(stresses[5], 2, False),
        differ(stresses[4], 0, False) + differ(stresses[5], 1, False) + differ(stresses[2], 2, True),
    ])
    return velocity + buoyancy * forces


def advance_stress(stresses, velocity, lame_first, rigidity):
    stretch_one = differ(velocity[0], 0, False)
    stretch_two = differ(velocity[1], 1, False)
    stretch_three = differ(velocity[2], 2, False)
    change = stretch_one + stretch_two + stretch_three
    rates = jnp.stack([
        lame_first * change + 2.0 * rigidity * stretch_one,
        lame_first * change + 2.0 * rigidity * stretch_two,
        lame_first * change + 2.0 * rigidity * stretch_three,
        rigidity * (differ(velocity[0], 1, True) + differ(velocity[1], 0, True)),
        rigidity * (differ(velocity[0], 2, True) + differ(velocity[2], 0, True)),
        rigidity * (differ(velocity[1], 2, True) + differ(velocity[2], 1, True)),
    ])
    return stresses + rates


def reference(velocity, stresses, buoyancy, lame_first, rigidity, histories, mechanism, resample, owners, cell_offsets):
    amplitude = jnp.dot(histories, resample, preferred_element_type=jnp.float32)
    terms = (mechanism.astype(jnp.float32)[:, :, None] * amplitude[:, None, :]).astype(jnp.bfloat16)
    device = jnp.arange(SOURCES, dtype=jnp.int32) // SRC_DEV
    across_cells = (device // N_GY) * CX + cell_offsets // (CY * CZ)
    normal_cells = owners[:, 0] * CY + (cell_offsets // CZ) % CY
    depth_cells = cell_offsets % CZ
    border = ((0, 0), (2, 2), (2, 2), (0, 0))
    for step_index in range(STEPS):
        velocity = advance_velocity(velocity, jnp.pad(stresses, border), buoyancy)
        stresses = advance_stress(stresses, jnp.pad(velocity, border), lame_first, rigidity)
        stresses = stresses.at[:, across_cells, normal_cells, depth_cells].add(terms[:, :, step_index].astype(jnp.float32).T)
    return velocity, stresses
```

```python
import jax
import jax.numpy as jnp
from jax import lax
from jax.experimental import pallas as pl
from jax.experimental.pallas import tpu as pltpu
from jax.sharding import PartitionSpec as P

INNER = 9.0 / 8.0
OUTER = -1.0 / 24.0
F32, BF16, I32 = jnp.float32, jnp.bfloat16, jnp.int32

N = 16
Z = 128
XO = 11
XE = XO + N + XO
YO = 16
YE = 48
DEPTH = [9] * 6 + [8] * 3 + [8, 6, 6]
CORNER = [8] * 6 + [6] * 3 + [6, 5, 5]
NQ = len(DEPTH)
FACE = [(q, d) for q in range(NQ) for d in range(1, DEPTH[q] + 1)]
FACE_AT = {qd: i for i, qd in enumerate(FACE)}
LOW_AT = {q: len(FACE) + q for q in range(NQ)}
NFACE = len(FACE) + NQ
CORN = [(q, d) for q in range(NQ) for d in range(1, CORNER[q] + 1)]
CORN_AT = {qd: NFACE + i for i, qd in enumerate(CORN)}
NCORN = len(CORN)
SLOTS = 64


def vmem():
    return pl.BlockSpec(memory_space=pltpu.VMEM)


def part(refs, q):
    v, s, b, l, m = refs
    if q < 6:
        return s.at[q]
    if q < 9:
        return v.at[q - 6]
    return (b, l, m)[q - 9]


def split(x):
    hi = x.astype(BF16)
    return hi, (x - hi.astype(F32)).astype(BF16)


def pack_y(v, s, b, l, m, out_a, out_b):
    odd = lax.rem(lax.axis_index("gy"), 2)
    refs = (v, s, b, l, m)
    for out, high in ((out_a, odd == 0), (out_b, odd == 1)):
        for q in range(NQ):
            src = part(refs, q)
            for d in range(1, DEPTH[q] + 1):
                y = jnp.where(high, N - d, d - 1)
                rows = src[pl.ds(y, N, stride=N), :]
                if d == 1:
                    hi, lo = split(rows)
                    out[FACE_AT[q, d]] = hi
                    out[LOW_AT[q]] = lo
                else:
                    out[FACE_AT[q, d]] = rows.astype(BF16)


def route(groups, hist, mech, res, owners, cells, out, vals):
    rows = hist.shape[0]
    nt = (((1,), (1,)), ((), ()))
    amp = lax.dot_general(res[...], hist[...], nt, preferred_element_type=F32)
    mechf = mech[...].astype(F32)
    vals[...] = jnp.zeros_like(vals)
    vals[0:6] = mechf * amp[0:1]
    vals[6:12] = mechf * amp[1:2]
    vals[16:22] = mechf * amp[2:3]
    cell = cells[...]
    vals[12:13] = (cell // Z).astype(F32)
    vals[13:14] = (cell % Z).astype(F32)
    v = vals[...].astype(BF16)
    own = owners[...]
    hits = (lax.broadcasted_iota(I32, (groups, rows), 0) == own).astype(F32)
    r0 = lax.broadcasted_iota(I32, (rows, rows), 0)
    r1 = lax.broadcasted_iota(I32, (rows, rows), 1)
    before = (r0 < r1).astype(F32).astype(BF16)
    earlier = jnp.dot(hits.astype(BF16), before, preferred_element_type=F32)
    rank = jnp.sum(hits * earlier, axis=0, keepdims=True)
    slot = own * SLOTS + rank.astype(I32)
    total = groups * SLOTS
    pick = (lax.broadcasted_iota(I32, (total, rows), 0) == slot).astype(F32).astype(BF16)
    sent = lax.dot_general(v, pick, nt, preferred_element_type=F32)
    turned = pltpu.roll(sent, SLOTS, 1)
    left = lax.broadcasted_iota(I32, (16, 2 * SLOTS), 1) < SLOTS
    zero = jnp.zeros((16, 2 * SLOTS), F32)

    def plain(j, h):
        return sent[16 * h : 16 * h + 16, 128 * j : 128 * j + 128]

    def shifted(j, h):
        j = j % (groups // 2)
        return turned[16 * h : 16 * h + 16, 128 * j : 128 * j + 128]

    for o in range(groups):
        j = o // 2
        if o % 2 == 0:
            sides = jnp.where(left, shifted(j, 0) if j else zero, plain(j, 0))
            mine = jnp.where(left, plain(j, 0), shifted(j, 1))
        else:
            last = o == groups - 1
            sides = jnp.where(left, plain(j, 0), zero if last else shifted(j + 1, 0))
            mine = jnp.where(left, shifted(j + 1, 0), plain(j, 1))
        out[o, 0:16, :] = sides.astype(BF16)
        out[o, 16:32, :] = mine.astype(BF16)


def pack_x(ya, yb, v, s, b, l, m, lists, out_a, out_b):
    odd_x = lax.rem(lax.axis_index("gx"), 2)
    odd_y = lax.rem(lax.axis_index("gy"), 2)
    refs = (v, s, b, l, m)
    for out, high in ((out_a, odd_x == 0), (out_b, odd_x == 1)):
        for q in range(NQ):
            src = part(refs, q)
            for d in range(1, DEPTH[q] + 1):
                x = jnp.where(high, N - d, d - 1)
                rows = src[pl.ds(pl.multiple_of(x * N, N), N), :]
                if d == 1:
                    hi, lo = split(rows)
                    out[FACE_AT[q, d]] = hi
                    out[LOW_AT[q]] = lo
                else:
                    out[FACE_AT[q, d]] = rows.astype(BF16)
        groups = lists.shape[0]
        for g in range(groups):
            for h in range(2):
                out[NFACE + NCORN + 2 * g + h] = lists[g, 16 * h : 16 * h + 16, :]

    def corners(low, top, out, high):
        for q, d in CORN:
            i = FACE_AT[q, d]
            a = low[i].astype(F32)
            c = top[i].astype(F32)
            k = 8 if high else 0
            both = jnp.concatenate([a[k : k + 8], c[k : k + 8]], axis=0)
            out[CORN_AT[q, d]] = both.astype(BF16)

    for px in range(2):
        for py in range(2):

            @pl.when((odd_x == px) & (odd_y == py))
            def _():
                low, top = (yb, ya) if py == 0 else (ya, yb)
                corners(low, top, out_a, px == 0)
                corners(low, top, out_b, px == 1)


def lanes(blocks):
    return jnp.concatenate(blocks, axis=1)


def own_lists(get, groups):
    left = lax.broadcasted_iota(I32, (16, 128), 1) < SLOTS
    first, last = [], []
    for i in range(groups // 2):
        a, b = get(2 * i), get(2 * i + 1)
        first.append(jnp.where(left, a, pltpu.roll(b, SLOTS, 1)))
        last.append(jnp.where(left, pltpu.roll(a, SLOTS, 1), b))
    return lanes(first), lanes(last)


def one_hot(code, count):
    width = code.shape[1]
    return (lax.broadcasted_iota(I32, (count, width), 0) == code).astype(F32).astype(BF16)


NT = (((1,), (1,)), ((), ()))


def place(planes, levels, values, row):
    a = planes * values[row : row + 1, :]
    return lax.dot_general(a, levels, NT, preferred_element_type=F32)


def sided(groups, sides):
    plane = sides[12:13, :].astype(I32)
    level = sides[13:14, :].astype(I32)
    upper = lax.rem(lax.broadcasted_iota(I32, plane.shape, 1), 128) >= SLOTS
    x, y = plane // N, plane % N
    row = jnp.where(upper, y, y - 8)
    row = jnp.where(upper, jnp.where(y <= 5, row, -9999), jnp.where(y >= 10, row, -9999))
    levels = one_hot(jnp.where(upper, level + Z, level), 2 * Z)
    return x, row, levels


def place_own(lists, out_own, out_side):
    groups = lists.shape[0]
    first, last = own_lists(lambda g: lists[g, 16:32, :].astype(F32), groups)
    planes = one_hot(first[12:13, :].astype(I32), N * N)
    levels = one_hot(first[13:14, :].astype(I32), Z)
    first, last = first.astype(BF16), last.astype(BF16)
    for t in range(3):
        for c in range(6):
            vals, row = (first, 6 * t + c) if t < 2 else (last, c)
            out_own[6 * t + c] = place(planes, levels, vals, row)
    sides = lanes([lists[g, 0:16, :].astype(F32) for g in range(groups)])
    x, row, levels = sided(groups, sides)
    planes = one_hot(x * 8 + row, 8 * N)
    sides = sides.astype(BF16)
    for k in range(12):
        out_side[k] = place(planes, levels, sides, k)


def roll_z(f, k, lane):
    moved = pltpu.roll(f, (-k) % Z, f.ndim - 1)
    keep = (lane < Z - k) if k > 0 else (lane >= -k)
    return jnp.where(keep, moved, 0.0)


def advance(xa, xb, ya, yb, v, s, b, l, m, own, side, vout, sout, ev, es, eb, el, em):
    odd_x = lax.rem(lax.axis_index("gx"), 2)
    odd_y = lax.rem(lax.axis_index("gy"), 2)
    refs = (v, s, b, l, m)
    ext = (ev, es, eb, el, em)

    def at(x, y):
        return x * YE + y

    for q in range(NQ):
        src, dst = part(refs, q), part(ext, q)
        for x in range(N):
            dst[at(XO + x, YO) : at(XO + x, YO) + N, :] = src[N * x : N * x + N, :]

    def layer(msg, q, d):
        rows = msg[FACE_AT[q, d]].astype(F32)
        if d == 1:
            rows = rows + msg[LOW_AT[q]].astype(F32)
        return rows

    def put_y(low, top):
        for q in range(NQ):
            dst = part(ext, q)
            for d in range(1, DEPTH[q] + 1):
                dst[pl.ds(at(XO, YO - d), N, stride=YE), :] = layer(low, q, d)
                dst[pl.ds(at(XO, YO + N - 1 + d), N, stride=YE), :] = layer(top, q, d)

    def put_x(low, top):
        groups = (low.shape[0] - NFACE - NCORN) // 2
        for q in range(NQ):
            dst = part(ext, q)
            for d in range(1, DEPTH[q] + 1):
                for msg, x in ((low, XO - d), (top, XO + N - 1 + d)):
                    dst[at(x, YO) : at(x, YO) + N, :] = layer(msg, q, d)
            for d in range(1, CORNER[q] + 1):
                for msg, x in ((low, XO - 8), (top, XO + N)):
                    both = msg[CORN_AT[q, d]].astype(F32)
                    dst[pl.ds(at(x, YO - d), 8, stride=YE), :] = both[0:8]
                    dst[pl.ds(at(x, YO + N - 1 + d), 8, stride=YE), :] = both[8:16]
        return groups

    for odd, put, one, two in ((odd_y, put_y, ya, yb), (odd_x, put_x, xa, xb)):

        @pl.when(odd == 0)
        def _():
            put(two, one)

        @pl.when(odd == 1)
        def _():
            put(one, two)

    def velocity_at(x, y0, n):
        base = x * YE
        lane = lax.broadcasted_iota(I32, (n, Z), 1)

        def st(c, dx=0, dy=0):
            return es[c, pl.ds(base + (dx * YE + y0 + dy), n), :]

        def dif(g, fwd):
            k = 0 if fwd else -1
            return INNER * (g(1 + k) - g(k)) + OUTER * (g(2 + k) - g(k - 1))

        def along_z(f):
            return lambda k: f if k == 0 else roll_z(f, k, lane)

        buoy = eb[pl.ds(base + y0, n), :]
        fx = dif(lambda k: st(0, dx=k), True) + dif(lambda k: st(3, dy=k), False)
        fx = fx + dif(along_z(st(4)), False)
        fy = dif(lambda k: st(3, dx=k), False) + dif(lambda k: st(1, dy=k), True)
        fy = fy + dif(along_z(st(5)), False)
        fz = dif(lambda k: st(4, dx=k), False) + dif(lambda k: st(5, dy=k), False)
        fz = fz + dif(along_z(st(2)), True)
        for c, f in enumerate((fx, fy, fz)):
            here = pl.ds(base + y0, n)
            ev[c, here, :] = ev[c, here, :] + buoy * f

    def stress_at(x, y0, n):
        base = x * YE
        lane = lax.broadcasted_iota(I32, (n, Z), 1)

        def ve(c, dx=0, dy=0):
            return ev[c, pl.ds(base + (dx * YE + y0 + dy), n), :]

        def dif(g, fwd):
            k = 0 if fwd else -1
            return INNER * (g(1 + k) - g(k)) + OUTER * (g(2 + k) - g(k - 1))

        def along_z(f):
            return lambda k: f if k == 0 else roll_z(f, k, lane)

        here = pl.ds(base + y0, n)
        lam, rig = el[here, :], em[here, :]
        d1 = dif(lambda k: ve(0, dx=k), False)
        d2 = dif(lambda k: ve(1, dy=k), False)
        d3 = dif(along_z(ve(2)), False)
        e = lam * (d1 + d2 + d3)
        two = 2.0 * rig
        rates = (
            e + two * d1,
            e + two * d2,
            e + two * d3,
            rig * (dif(lambda k: ve(0, dy=k), True) + dif(lambda k: ve(1, dx=k), True)),
            rig * (dif(along_z(ve(0)), True) + dif(lambda k: ve(2, dx=k), True)),
            rig * (dif(along_z(ve(1)), True) + dif(lambda k: ve(2, dy=k), True)),
        )
        for c, r in enumerate(rates):
            es[c, here, :] = es[c, here, :] + r

    def sweep(fn, reach, y0, n):
        def step(x, carry):
            fn(x, y0, n)
            return carry

        lax.fori_loop(XO - reach, XO + N + reach, step, 0)

    def add(c, x, y, rows):
        here = slice(at(x, y), at(x, y) + rows.shape[0])
        es[c, here, :] = es[c, here, :] + rows

    def add_own(t):
        for c in range(6):
            for x in range(N):
                add(c, XO + x, YO, own[6 * t + c, N * x : N * x + N, :])

    def add_side(t):
        for c in range(6):
            for x in range(N):
                rows = slice(8 * x, 8 * x + 8)
                add(c, XO + x, YO - 8, side[6 * t + c, rows, 0:Z])
                add(c, XO + x, YO + N, side[6 * t + c, rows, Z : 2 * Z])

    def add_beyond(t, far):
        groups = (xa.shape[0] - NFACE - NCORN) // 2
        base = NFACE + NCORN

        def one(msg, up):
            first, _ = own_lists(lambda g: msg[base + 2 * g + 1].astype(F32), groups)
            plane = first[12:13, :].astype(I32)
            levels = one_hot(first[13:14, :].astype(I32), Z)
            x, y = plane // N, plane % N
            i = x if up else x - (N - far)
            planes = one_hot(jnp.where(i >= 0, i * N + y, -1), far * N)
            first = first.astype(BF16)
            x0 = XO + N if up else XO - far
            for c in range(6):
                got = place(planes, levels, first, 6 * t + c)
                for k in range(far):
                    add(c, x0 + k, YO, got[N * k : N * k + N])
            near = 5 if t == 0 else 2
            sides = lanes([msg[base + 2 * g].astype(F32) for g in range(groups)])
            x, row, levels = sided(groups, sides)
            i = x if up else x - (N - near)
            planes = one_hot(jnp.where(i >= 0, i * 8 + row, -1), 8 * near)
            sides = sides.astype(BF16)
            x0 = XO + N if up else XO - near
            for c in range(6):
                got = place(planes, levels, sides, 6 * t + c)
                for k in range(near):
                    add(c, x0 + k, YO - 8, got[8 * k : 8 * k + 8, 0:Z])
                    add(c, x0 + k, YO + N, got[8 * k : 8 * k + 8, Z : 2 * Z])

        @pl.when(odd_x == 0)
        def _():
            one(xb, False)
            one(xa, True)

        @pl.when(odd_x == 1)
        def _():
            one(xa, False)
            one(xb, True)

    sweep(velocity_at, 8, 8, 32)
    sweep(stress_at, 6, 8, 32)
    add_own(0)
    add_side(0)
    add_beyond(0, 6)
    sweep(velocity_at, 5, 8, 32)
    sweep(stress_at, 3, 8, 32)
    add_own(1)
    add_side(1)
    add_beyond(1, 3)
    sweep(velocity_at, 2, 8, 32)
    sweep(stress_at, 0, 16, 16)
    for x in range(N):
        here = slice(at(XO + x, YO), at(XO + x, YO) + N)
        rows = slice(N * x, N * x + N)
        for c in range(3):
            vout[c, rows, :] = ev[c, here, :]
        for c in range(6):
            sout[c, rows, :] = es[c, here, :] + own[12 + c, rows, :]


def swaps(count, first):
    pairs = []
    for i in range(first, count - 1, 2):
        pairs += [(i, i + 1), (i + 1, i)]
    return pairs


def swap_both(a, b, axis):
    count = lax.axis_size(axis)
    return (
        lax.ppermute(a, axis, swaps(count, 0)),
        lax.ppermute(b, axis, swaps(count, 1)),
    )


def call(kernel, outs, args, scratch=(), flops=1_000_000):
    return pl.pallas_call(
        kernel,
        out_shape=[jax.ShapeDtypeStruct(s, t) for s, t in outs],
        in_specs=[vmem()] * len(args),
        out_specs=[vmem()] * len(outs),
        scratch_shapes=list(scratch),
        compiler_params=pltpu.CompilerParams(vmem_limit_bytes=56 * 1024 * 1024),
        cost_estimate=pl.CostEstimate(flops=flops, bytes_accessed=1_000_000, transcendentals=0),
    )(*args)


def local(velocity, stresses, buoyancy, lame, rigidity, hist, mech, res, owners, cells):
    groups = lax.axis_size("gy")
    v = velocity.reshape(3, N * N, Z)
    s = stresses.reshape(6, N * N, Z)
    b, l, m = (a.reshape(N * N, Z) for a in (buoyancy, lame, rigidity))
    state = (v, s, b, l, m)
    face = ((NFACE, N, Z), BF16)
    ya, yb = call(pack_y, [face, face], state)
    ya, yb = swap_both(ya, yb, "gy")
    rows = hist.shape[0]
    (sent,) = call(
        lambda *refs: route(groups, *refs),
        [((groups, 32, 128), BF16)],
        (hist, mech.T, res.T, owners.reshape(1, rows), cells.reshape(1, rows)),
        [pltpu.VMEM((32, rows), F32)],
    )
    lists = lax.all_to_all(sent, "gy", split_axis=0, concat_axis=0, tiled=True)
    whole = ((NFACE + NCORN + 2 * groups, N, Z), BF16)
    xa, xb = call(pack_x, [whole, whole], (ya, yb) + state + (lists,))
    xa, xb = swap_both(xa, xb, "gx")
    own, side = call(
        place_own,
        [((18, N * N, Z), F32), ((12, 8 * N, 2 * Z), F32)],
        (lists,),
        flops=10_000_000_000,
    )
    block = pltpu.VMEM((XE * YE, Z), F32)
    vout, sout = call(
        advance,
        [(v.shape, F32), (s.shape, F32)],
        (xa, xb, ya, yb) + state + (own, side),
        [pltpu.VMEM((3, XE * YE, Z), F32), pltpu.VMEM((6, XE * YE, Z), F32), block, block, block],
    )
    return vout.reshape(velocity.shape), sout.reshape(stresses.shape)


def solution(mesh):
    in_specs = (
        P(None, "gx", "gy", None),
        P(None, "gx", "gy", None),
        P("gx", "gy", None),
        P("gx", "gy", None),
        P("gx", "gy", None),
        P(("gx", "gy"), None),
        P(("gx", "gy"), None),
        P(),
        P(("gx", "gy"), None),
        P(("gx", "gy")),
    )
    out_specs = (P(None, "gx", "gy", None), P(None, "gx", "gy", None))
    return jax.shard_map(local, mesh=mesh, in_specs=in_specs, out_specs=out_specs, check_vma=False)
```

```python
import jax
import jax.numpy as jnp
from jax import lax
from jax.experimental import pallas as pl
from jax.experimental.pallas import tpu as pltpu
from jax.sharding import PartitionSpec as P

INNER = 9.0 / 8.0
OUTER = -1.0 / 24.0
F32, BF16, I32 = jnp.float32, jnp.bfloat16, jnp.int32

N = 16
Z = 128
XO = 11
XE = XO + N + XO
YO = 16
YE = 48
DEPTH = [9] * 6 + [8] * 3 + [8, 6, 6]
CORNER = [8] * 6 + [6] * 3 + [6, 5, 5]
NQ = len(DEPTH)
FACE = [(q, d) for q in range(NQ) for d in range(1, DEPTH[q] + 1)]
FACE_AT = {qd: i for i, qd in enumerate(FACE)}
LOW_AT = {q: len(FACE) + q for q in range(NQ)}
NFACE = len(FACE) + NQ
CORN = [(q, d) for q in range(NQ) for d in range(1, CORNER[q] + 1)]
CORN_AT = {qd: NFACE + i for i, qd in enumerate(CORN)}
NCORN = len(CORN)
SLOTS = 64
UNROLL = 4
FIRST = 61
SECOND = 61
FAR = (6, 3)
NEAR = (5, 2)


def vmem():
    return pl.BlockSpec(memory_space=pltpu.VMEM)


def part(refs, q):
    v, s, b, l, m = refs
    if q < 6:
        return s.at[q]
    if q < 9:
        return v.at[q - 6]
    return (b, l, m)[q - 9]


def split(x):
    hi = x.astype(BF16)
    return hi, (x - hi.astype(F32)).astype(BF16)


def fetch(pairs, sems):
    copies = [pltpu.make_async_copy(a, b, sems.at[i]) for i, (a, b) in enumerate(pairs)]
    for copy in copies:
        copy.start()
    return copies


def pack_y(v_in, s_in, b_in, l_in, m_in, out_a, out_b, v, s, b, l, m, sems):
    copies = fetch([(s_in, s), (v_in, v), (b_in, b), (l_in, l), (m_in, m)], sems)
    for copy in copies:
        copy.wait()
    odd = lax.rem(lax.axis_index("gy"), 2)
    refs = (v, s, b, l, m)
    for out, high in ((out_a, odd == 0), (out_b, odd == 1)):
        for q in range(NQ):
            src = part(refs, q)
            for d in range(1, DEPTH[q] + 1):
                y = jnp.where(high, N - d, d - 1)
                rows = src[pl.ds(y, N, stride=N), :]
                if d == 1:
                    hi, lo = split(rows)
                    out[FACE_AT[q, d]] = hi
                    out[LOW_AT[q]] = lo
                else:
                    out[FACE_AT[q, d]] = rows.astype(BF16)


def route(groups, *refs):
    given, out, held, vals, sems = refs[:5], refs[5], refs[6:11], refs[11], refs[12]
    for copy in fetch(list(zip(given, held)), sems):
        copy.wait()
    hist, mech, res, owners, cells = held
    rows = hist.shape[0]
    nt = (((1,), (1,)), ((), ()))
    amp = lax.dot_general(res[...], hist[...], nt, preferred_element_type=F32)
    mechf = mech[...].astype(F32)
    vals[...] = jnp.zeros_like(vals)
    vals[0:6] = mechf * amp[0:1]
    vals[6:12] = mechf * amp[1:2]
    vals[16:22] = mechf * amp[2:3]
    cell = cells[...]
    vals[12:13] = (cell // Z).astype(F32)
    vals[13:14] = (cell % Z).astype(F32)
    v = vals[...].astype(BF16)
    own = owners[...]
    hits = (lax.broadcasted_iota(I32, (groups, rows), 0) == own).astype(F32)
    r0 = lax.broadcasted_iota(I32, (rows, rows), 0)
    r1 = lax.broadcasted_iota(I32, (rows, rows), 1)
    before = (r0 < r1).astype(F32).astype(BF16)
    earlier = jnp.dot(hits.astype(BF16), before, preferred_element_type=F32)
    rank = jnp.sum(hits * earlier, axis=0, keepdims=True)
    slot = own * SLOTS + rank.astype(I32)
    total = groups * SLOTS
    pick = (lax.broadcasted_iota(I32, (total, rows), 0) == slot).astype(F32).astype(BF16)
    sent = lax.dot_general(v, pick, nt, preferred_element_type=F32)
    turned = pltpu.roll(sent, SLOTS, 1)
    left = lax.broadcasted_iota(I32, (16, 2 * SLOTS), 1) < SLOTS
    zero = jnp.zeros((16, 2 * SLOTS), F32)

    def plain(j, h):
        return sent[16 * h : 16 * h + 16, 128 * j : 128 * j + 128]

    def shifted(j, h):
        j = j % (groups // 2)
        return turned[16 * h : 16 * h + 16, 128 * j : 128 * j + 128]

    for o in range(groups):
        j = o // 2
        if o % 2 == 0:
            sides = jnp.where(left, shifted(j, 0) if j else zero, plain(j, 0))
            mine = jnp.where(left, plain(j, 0), shifted(j, 1))
        else:
            last = o == groups - 1
            sides = jnp.where(left, plain(j, 0), zero if last else shifted(j + 1, 0))
            mine = jnp.where(left, shifted(j + 1, 0), plain(j, 1))
        out[o, 0:16, :] = sides.astype(BF16)
        out[o, 16:32, :] = mine.astype(BF16)


def pack_x(ya, yb, v, s, mats, lists, out_a, out_b):
    odd_x = lax.rem(lax.axis_index("gx"), 2)
    odd_y = lax.rem(lax.axis_index("gy"), 2)
    refs = (v, s, mats.at[0], mats.at[1], mats.at[2])
    for out, high in ((out_a, odd_x == 0), (out_b, odd_x == 1)):
        for q in range(NQ):
            src = part(refs, q)
            for d in range(1, DEPTH[q] + 1):
                x = jnp.where(high, N - d, d - 1)
                rows = src[pl.ds(pl.multiple_of(x * N, N), N), :]
                if d == 1:
                    hi, lo = split(rows)
                    out[FACE_AT[q, d]] = hi
                    out[LOW_AT[q]] = lo
                else:
                    out[FACE_AT[q, d]] = rows.astype(BF16)
        groups = lists.shape[0]
        for g in range(groups):
            for h in range(2):
                out[NFACE + NCORN + 2 * g + h] = lists[g, 16 * h : 16 * h + 16, :]

    def corners(low, top, out, high):
        for q, d in CORN:
            i = FACE_AT[q, d]
            a = low[i].astype(F32)
            c = top[i].astype(F32)
            k = 8 if high else 0
            both = jnp.concatenate([a[k : k + 8], c[k : k + 8]], axis=0)
            out[CORN_AT[q, d]] = both.astype(BF16)

    for px in range(2):
        for py in range(2):

            @pl.when((odd_x == px) & (odd_y == py))
            def _():
                low, top = (yb, ya) if py == 0 else (ya, yb)
                corners(low, top, out_a, px == 0)
                corners(low, top, out_b, px == 1)


def lanes(blocks):
    return jnp.concatenate(blocks, axis=1)


def own_lists(get, groups):
    left = lax.broadcasted_iota(I32, (16, 128), 1) < SLOTS
    first, last = [], []
    for i in range(groups // 2):
        a, b = get(2 * i), get(2 * i + 1)
        first.append(jnp.where(left, a, pltpu.roll(b, SLOTS, 1)))
        last.append(jnp.where(left, pltpu.roll(a, SLOTS, 1), b))
    return lanes(first), lanes(last)


def one_hot(code, count):
    width = code.shape[1]
    return (lax.broadcasted_iota(I32, (count, width), 0) == code).astype(F32).astype(BF16)


NT = (((1,), (1,)), ((), ()))


def place(parts, values, levels):
    a = [p * values[r + c : r + c + 1, :] for p, r in parts for c in range(6)]
    return lax.dot_general(jnp.concatenate(a, axis=0), levels, NT, preferred_element_type=F32)


def sided(groups, sides):
    plane = sides[12:13, :].astype(I32)
    level = sides[13:14, :].astype(I32)
    upper = lax.rem(lax.broadcasted_iota(I32, plane.shape, 1), 128) >= SLOTS
    x, y = plane // N, plane % N
    row = jnp.where(upper, y, y - 8)
    row = jnp.where(upper, jnp.where(y <= 5, row, -9999), jnp.where(y >= 10, row, -9999))
    levels = one_hot(jnp.where(upper, level + Z, level), 2 * Z)
    return x, row, levels


def place_own(lists, out_own, out_side):
    groups = lists.shape[0]
    first, last = own_lists(lambda g: lists[g, 16:32, :].astype(F32), groups)
    planes = one_hot(first[12:13, :].astype(I32), N * N)
    levels = one_hot(first[13:14, :].astype(I32), Z)
    first, last = first.astype(BF16), last.astype(BF16)
    for t in range(3):
        vals, row = (first, 6 * t) if t < 2 else (last, 0)
        spread = [levels * vals[row + c : row + c + 1, :] for c in range(6)]
        got = lax.dot_general(planes, jnp.concatenate(spread, axis=0), NT, preferred_element_type=F32)
        for c in range(6):
            out_own[6 * t + c] = got[:, Z * c : Z * c + Z]
    sides = lanes([lists[g, 0:16, :].astype(F32) for g in range(groups)])
    x, row, levels = sided(groups, sides)
    planes = one_hot(x * 8 + row, 8 * N)
    sides = sides.astype(BF16)
    got = place(((planes, 0), (planes, 6)), sides, levels)
    for k in range(12):
        out_side[k] = got[8 * N * k : 8 * N * k + 8 * N]


def roll_z(f, k, lane):
    moved = pltpu.roll(f, (-k) % Z, f.ndim - 1)
    keep = (lane < Z - k) if k > 0 else (lane >= -k)
    return jnp.where(keep, moved, 0.0)


def advance(xa, xb, ya, yb, v, s, mats, own, side, vout, sout, ev, es, eb, el, em, beyond, corner):
    odd_x = lax.rem(lax.axis_index("gx"), 2)
    odd_y = lax.rem(lax.axis_index("gy"), 2)
    refs = (v, s, mats.at[0], mats.at[1], mats.at[2])
    ext = (ev, es, eb, el, em)

    def at(x, y):
        return x * YE + y

    for q in range(NQ):
        src, dst = part(refs, q), part(ext, q)
        for x in range(N):
            dst[at(XO + x, YO) : at(XO + x, YO) + N, :] = src[N * x : N * x + N, :]

    def layer(msg, q, d):
        rows = msg[FACE_AT[q, d]].astype(F32)
        if d == 1:
            rows = rows + msg[LOW_AT[q]].astype(F32)
        return rows

    def put_y(low, top):
        for q in range(NQ):
            dst = part(ext, q)
            for d in range(1, DEPTH[q] + 1):
                dst[pl.ds(at(XO, YO - d), N, stride=YE), :] = layer(low, q, d)
                dst[pl.ds(at(XO, YO + N - 1 + d), N, stride=YE), :] = layer(top, q, d)

    def put_x(low, top):
        groups = (low.shape[0] - NFACE - NCORN) // 2
        for q in range(NQ):
            dst = part(ext, q)
            for d in range(1, DEPTH[q] + 1):
                for msg, x in ((low, XO - d), (top, XO + N - 1 + d)):
                    dst[at(x, YO) : at(x, YO) + N, :] = layer(msg, q, d)
            for d in range(1, CORNER[q] + 1):
                for msg, x in ((low, XO - 8), (top, XO + N)):
                    both = msg[CORN_AT[q, d]].astype(F32)
                    dst[pl.ds(at(x, YO - d), 8, stride=YE), :] = both[0:8]
                    dst[pl.ds(at(x, YO + N - 1 + d), 8, stride=YE), :] = both[8:16]
        return groups

    for odd, put, one, two in ((odd_y, put_y, ya, yb), (odd_x, put_x, xa, xb)):

        @pl.when(odd == 0)
        def _():
            put(two, one)

        @pl.when(odd == 1)
        def _():
            put(one, two)

    def total(terms):
        near = far = None
        for g, fwd in terms:
            k = 0 if fwd else -1
            p, q = g(1 + k) - g(k), g(2 + k) - g(k - 1)
            near, far = (p, q) if near is None else (near + p, far + q)
        return INNER * near + OUTER * far

    def reader(ref, x, y0, n):
        base = pl.multiple_of(x * YE, 8)

        def along_x(c):
            return lambda k: ref[c, pl.ds(base + (k * YE + y0), n), :]

        def along_y(c):
            return lambda k: ref[c, pl.ds(base + (y0 + k), n), :]

        def along_z(c):
            f = ref[c, pl.ds(base + y0, n), :]
            lane = lax.broadcasted_iota(I32, (n, Z), 1)
            return lambda k: f if k == 0 else roll_z(f, k, lane)

        return along_x, along_y, along_z, pl.ds(base + y0, n)

    def velocity_at(x, y0, n):
        ax, ay, az, here = reader(es, x, y0, n)
        buoy = eb[here, :]
        forces = (
            total(((ax(0), True), (ay(3), False), (az(4), False))),
            total(((ax(3), False), (ay(1), True), (az(5), False))),
            total(((ax(4), False), (ay(5), False), (az(2), True))),
        )
        for c, f in enumerate(forces):
            ev[c, here, :] = ev[c, here, :] + buoy * f

    def stress_at(x, y0, n):
        ax, ay, az, here = reader(ev, x, y0, n)
        lam, rig = el[here, :], em[here, :]
        d1, d2, d3 = total(((ax(0), False),)), total(((ay(1), False),)), total(((az(2), False),))
        e = lam * (d1 + d2 + d3)
        two = 2.0 * rig
        rates = (
            e + two * d1,
            e + two * d2,
            e + two * d3,
            rig * total(((ay(0), True), (ax(1), True))),
            rig * total(((az(0), True), (ax(2), True))),
            rig * total(((az(1), True), (ay(2), True))),
        )
        for c, r in enumerate(rates):
            es[c, here, :] = es[c, here, :] + r

    def sweep(fn, reach, y0, n):
        def step(x, carry):
            fn(x, y0, n)
            return carry

        lax.fori_loop(XO - reach, XO + N + reach, step, 0, unroll=UNROLL)

    def add(c, x, y, rows):
        here = slice(at(x, y), at(x, y) + rows.shape[0])
        es[c, here, :] = es[c, here, :] + rows

    def add_own(t):
        for c in range(6):
            for x in range(N):
                add(c, XO + x, YO, own[6 * t + c, N * x : N * x + N, :])

    def add_side(t):
        for c in range(6):
            for x in range(N):
                rows = slice(8 * x, 8 * x + 8)
                add(c, XO + x, YO - 8, side[6 * t + c, rows, 0:Z])
                add(c, XO + x, YO + N, side[6 * t + c, rows, Z : 2 * Z])

    def place_beyond():
        groups = (xa.shape[0] - NFACE - NCORN) // 2
        base = NFACE + NCORN

        def one(msg, up, k):
            first, _ = own_lists(lambda g: msg[base + 2 * g + 1].astype(F32), groups)
            plane = first[12:13, :].astype(I32)
            levels = one_hot(first[13:14, :].astype(I32), Z)
            x, y = plane // N, plane % N

            def faces(far):
                i = x if up else x - (N - far)
                return one_hot(jnp.where(i >= 0, i * N + y, -1), far * N)

            parts = ((faces(FAR[0]), 0), (faces(FAR[1]), 6))
            beyond[k] = place(parts, first.astype(BF16), levels)
            sides = lanes([msg[base + 2 * g].astype(F32) for g in range(groups)])
            sx, row, levels = sided(groups, sides)

            def edges(near):
                i = sx if up else sx - (N - near)
                return one_hot(jnp.where(i >= 0, i * 8 + row, -1), 8 * near)

            parts = ((edges(NEAR[0]), 0), (edges(NEAR[1]), 6))
            corner[k] = place(parts, sides.astype(BF16), levels)

        @pl.when(odd_x == 0)
        def _():
            one(xb, False, 0)
            one(xa, True, 1)

        @pl.when(odd_x == 1)
        def _():
            one(xa, False, 0)
            one(xb, True, 1)

    def add_beyond(t):
        far, near = FAR[t], NEAR[t]
        f0, n0 = (0, 0) if t == 0 else (6 * N * FAR[0], 6 * 8 * NEAR[0])
        for k in range(2):
            for c in range(6):
                x0 = XO + N if k else XO - far
                for i in range(far):
                    r = f0 + N * (c * far + i)
                    add(c, x0 + i, YO, beyond[k, r : r + N, :])
                x0 = XO + N if k else XO - near
                for i in range(near):
                    r = n0 + 8 * (c * near + i)
                    add(c, x0 + i, YO - 8, corner[k, r : r + 8, 0:Z])
                    add(c, x0 + i, YO + N, corner[k, r : r + 8, Z : 2 * Z])

    place_beyond()
    sweep(velocity_at, 8, 8, 32)
    sweep(stress_at, 6, 8, 32)
    add_own(0)
    add_side(0)
    add_beyond(0)
    sweep(velocity_at, 5, 8, 32)
    sweep(stress_at, 3, 13, 24)
    add_own(1)
    add_side(1)
    add_beyond(1)
    sweep(velocity_at, 2, 14, 24)
    sweep(stress_at, 0, 16, 16)
    for x in range(N):
        here = slice(at(XO + x, YO), at(XO + x, YO) + N)
        rows = slice(N * x, N * x + N)
        for c in range(3):
            vout[c, rows, :] = ev[c, here, :]
        for c in range(6):
            sout[c, rows, :] = es[c, here, :] + own[12 + c, rows, :]


SCRATCH = [pltpu.VMEM((n, XE * YE, Z), F32) for n in (3, 6)] + [pltpu.VMEM((XE * YE, Z), F32)] * 3
SCRATCH += [
    pltpu.VMEM((2, 6 * N * (FAR[0] + FAR[1]), Z), F32),
    pltpu.VMEM((2, 6 * 8 * (NEAR[0] + NEAR[1]), 2 * Z), F32),
]


def swaps(count, first):
    pairs = []
    for i in range(first, count - 1, 2):
        pairs += [(i, i + 1), (i + 1, i)]
    return pairs


def swap_both(a, b, axis):
    count = lax.axis_size(axis)
    return (
        lax.ppermute(a, axis, swaps(count, 0)),
        lax.ppermute(b, axis, swaps(count, 1)),
    )


def call(kernel, outs, args, scratch=(), flops=1_000_000, mib=8, here=True):
    if not here:
        held = [pltpu.VMEM(a.shape, a.dtype) for a in args]
        scratch = held + list(scratch) + [pltpu.SemaphoreType.DMA((len(args),))]
    return pl.pallas_call(
        kernel,
        out_shape=[jax.ShapeDtypeStruct(s, t) for s, t in outs],
        in_specs=[vmem() if here else pl.BlockSpec(memory_space=pltpu.HBM)] * len(args),
        out_specs=[vmem()] * len(outs),
        scratch_shapes=list(scratch),
        compiler_params=pltpu.CompilerParams(vmem_limit_bytes=mib * 1024 * 1024),
        cost_estimate=pl.CostEstimate(flops=flops, bytes_accessed=1_000_000, transcendentals=0),
    )(*args)


def local(velocity, stresses, buoyancy, lame, rigidity, hist, mech, res, owners, cells):
    groups = lax.axis_size("gy")
    v = velocity.reshape(3, N * N, Z)
    s = stresses.reshape(6, N * N, Z)
    b, l, m = (a.reshape(N * N, Z) for a in (buoyancy, lame, rigidity))
    state = (v, s, b, l, m)
    mats = jnp.stack([b, l, m])
    later = (v, s, mats)
    face = ((NFACE, N, Z), BF16)
    ya, yb = call(pack_y, [face, face], state, here=False, mib=FIRST)
    ya, yb = swap_both(ya, yb, "gy")
    rows = hist.shape[0]
    (sent,) = call(
        lambda *refs: route(groups, *refs),
        [((groups, 32, 128), BF16)],
        (hist, mech.T, res.T, owners.reshape(1, rows), cells.reshape(1, rows)),
        [pltpu.VMEM((32, rows), F32)],
        here=False,
        mib=SECOND,
    )
    lists = lax.all_to_all(sent, "gy", split_axis=0, concat_axis=0, tiled=True)
    whole = ((NFACE + NCORN + 2 * groups, N, Z), BF16)
    xa, xb = call(pack_x, [whole, whole], (ya, yb) + later + (lists,))
    xa, xb = swap_both(xa, xb, "gx")
    own, side = call(
        place_own,
        [((18, N * N, Z), F32), ((12, 8 * N, 2 * Z), F32)],
        (lists,),
        flops=10_000_000_000,
        mib=24,
    )
    vout, sout = call(
        advance,
        [(v.shape, F32), (s.shape, F32)],
        (xa, xb, ya, yb) + later + (own, side),
        SCRATCH,
        mib=32,
    )
    return vout.reshape(velocity.shape), sout.reshape(stresses.shape)


def solution(mesh):
    in_specs = (
        P(None, "gx", "gy", None),
        P(None, "gx", "gy", None),
        P("gx", "gy", None),
        P("gx", "gy", None),
        P("gx", "gy", None),
        P(("gx", "gy"), None),
        P(("gx", "gy"), None),
        P(),
        P(("gx", "gy"), None),
        P(("gx", "gy")),
    )
    out_specs = (P(None, "gx", "gy", None), P(None, "gx", "gy", None))
    return jax.shard_map(local, mesh=mesh, in_specs=in_specs, out_specs=out_specs, check_vma=False)
```

```python
import jax
import jax.numpy as jnp
from jax import lax
from jax.experimental import pallas as pl
from jax.experimental.pallas import tpu as pltpu
from jax.sharding import PartitionSpec as P

INNER = 9.0 / 8.0
OUTER = -1.0 / 24.0
F32, BF16, I32 = jnp.float32, jnp.bfloat16, jnp.int32

N = 16
Z = 128
XO = 11
XE = XO + N + 10
YO = 16
YE = 40
DEPTH = [9] * 6 + [8] * 3 + [8, 6, 6]
CORNER = [8] * 6 + [6] * 3 + [6, 5, 5]
NQ = len(DEPTH)
FACE = [(q, d) for q in range(NQ) for d in range(1, DEPTH[q] + 1)]
FACE_AT = {qd: i for i, qd in enumerate(FACE)}
LOW_AT = {q: len(FACE) + q for q in range(NQ)}
NFACE = len(FACE) + NQ
PACKED = {
    8: ((1, 0, 0), (2, 0, 0), (3, 7, 2), (4, 6, 3), (5, 8, 2)),
    6: ((1, 6, 2), (2, 0, 0), (3, 4, 3), (5, 0, 0)),
    5: ((1, 3, 3), (2, 4, 2), (5, 0, 0)),
}
CORN = [(q,) + unit for q in range(NQ) for unit in PACKED[CORNER[q]]]
NCORN = len(CORN)
SLOTS = 64
UNROLL = {8: 8, 6: 7, 5: 13, 3: 11, 2: 10, 0: 8}
FIRST = 61
FAR = (6, 3)
NEAR = (5, 2)


def vmem():
    return pl.BlockSpec(memory_space=pltpu.VMEM)


def part(refs, q):
    v, s, b, l, m = refs
    if q < 6:
        return s.at[q]
    if q < 9:
        return v.at[q - 6]
    return (b, l, m)[q - 9]


def split(x):
    hi = x.astype(BF16)
    return hi, (x - hi.astype(F32)).astype(BF16)


def fetch(pairs, sems):
    copies = [pltpu.make_async_copy(a, b, sems.at[i]) for i, (a, b) in enumerate(pairs)]
    for copy in copies:
        copy.start()
    return copies


def opening(groups, *refs):
    given, (out_a, out_b, sent), held, vals, sems = refs[:10], refs[10:13], refs[13:23], refs[23], refs[24]
    copies = fetch(list(zip(given, held)), sems)
    for copy in copies[5:]:
        copy.wait()
    route(groups, *held[5:], sent, vals)
    for copy in copies[:5]:
        copy.wait()
    pack_y(*held[:5], out_a, out_b)


def pack_y(v, s, b, l, m, out_a, out_b):
    odd = lax.rem(lax.axis_index("gy"), 2)
    refs = (v, s, b, l, m)
    for out, high in ((out_a, odd == 0), (out_b, odd == 1)):
        for q in range(NQ):
            src = part(refs, q)
            for d in range(1, DEPTH[q] + 1):
                y = jnp.where(high, N - d, d - 1)
                rows = src[pl.ds(y, N, stride=N), :]
                if d == 1:
                    hi, lo = split(rows)
                    out[FACE_AT[q, d]] = hi
                    out[LOW_AT[q]] = lo
                else:
                    out[FACE_AT[q, d]] = rows.astype(BF16)


def route(groups, hist, mech, res, owners, cells, out, vals):
    rows = hist.shape[0]
    nt = (((1,), (1,)), ((), ()))
    amp = lax.dot_general(res[...], hist[...], nt, preferred_element_type=F32)
    mechf = mech[...].astype(F32)
    vals[...] = jnp.zeros_like(vals)
    vals[0:6] = mechf * amp[0:1]
    vals[6:12] = mechf * amp[1:2]
    vals[16:22] = mechf * amp[2:3]
    cell = cells[...]
    vals[12:13] = (cell // Z).astype(F32)
    vals[13:14] = (cell % Z).astype(F32)
    v = vals[...].astype(BF16)
    own = owners[...]
    hits = (lax.broadcasted_iota(I32, (groups, rows), 0) == own).astype(F32)
    r0 = lax.broadcasted_iota(I32, (rows, rows), 0)
    r1 = lax.broadcasted_iota(I32, (rows, rows), 1)
    before = (r0 < r1).astype(F32).astype(BF16)
    earlier = jnp.dot(hits.astype(BF16), before, preferred_element_type=F32)
    rank = jnp.sum(hits * earlier, axis=0, keepdims=True)
    slot = own * SLOTS + rank.astype(I32)
    total = groups * SLOTS
    pick = (lax.broadcasted_iota(I32, (total, rows), 0) == slot).astype(F32).astype(BF16)
    sent = lax.dot_general(v, pick, nt, preferred_element_type=F32)
    turned = pltpu.roll(sent, SLOTS, 1)
    left = lax.broadcasted_iota(I32, (16, 2 * SLOTS), 1) < SLOTS
    zero = jnp.zeros((16, 2 * SLOTS), F32)

    def plain(j, h):
        return sent[16 * h : 16 * h + 16, 128 * j : 128 * j + 128]

    def shifted(j, h):
        j = j % (groups // 2)
        return turned[16 * h : 16 * h + 16, 128 * j : 128 * j + 128]

    for o in range(groups):
        j = o // 2
        if o % 2 == 0:
            sides = jnp.where(left, shifted(j, 0) if j else zero, plain(j, 0))
            mine = jnp.where(left, plain(j, 0), shifted(j, 1))
        else:
            last = o == groups - 1
            sides = jnp.where(left, plain(j, 0), zero if last else shifted(j + 1, 0))
            mine = jnp.where(left, shifted(j + 1, 0), plain(j, 1))
        out[o, 0:16, :] = sides.astype(BF16)
        out[o, 16:32, :] = mine.astype(BF16)


def pack_x(v, s, mats, out_a, out_b):
    odd = lax.rem(lax.axis_index("gx"), 2)
    refs = (v, s, mats.at[0], mats.at[1], mats.at[2])
    for out, high in ((out_a, odd == 0), (out_b, odd == 1)):
        for q in range(NQ):
            src = part(refs, q)
            for d in range(1, DEPTH[q] + 1):
                x = jnp.where(high, N - d, d - 1)
                rows = src[pl.ds(pl.multiple_of(x * N, N), N), :]
                if d == 1:
                    hi, lo = split(rows)
                    out[FACE_AT[q, d]] = hi
                    out[LOW_AT[q]] = lo
                else:
                    out[FACE_AT[q, d]] = rows.astype(BF16)


def pack_corners(ya, yb, lists, out_a, out_b):
    odd_x = lax.rem(lax.axis_index("gx"), 2)
    odd_y = lax.rem(lax.axis_index("gy"), 2)
    groups = lists.shape[0]
    for out in (out_a, out_b):
        for g in range(groups):
            for h in range(2):
                out[NCORN + 2 * g + h] = lists[g, 16 * h : 16 * h + 16, :]

    def corners(low, top, out, high):
        row = lax.broadcasted_iota(I32, (8, Z), 0)
        k = 8 if high else 0
        for i, (q, d, far, m) in enumerate(CORN):
            halves = []
            for msg in (low, top):
                a = msg[FACE_AT[q, d]].astype(F32)[k : k + 8]
                if far:
                    c = msg[FACE_AT[q, far]].astype(F32)[k : k + 8]
                    if high:
                        a = jnp.where(row < m, pltpu.roll(c, m, 0), a)
                    else:
                        a = jnp.where(row >= 8 - m, pltpu.roll(c, 8 - m, 0), a)
                halves.append(a)
            out[i] = jnp.concatenate(halves, axis=0).astype(BF16)

    for px in range(2):
        for py in range(2):

            @pl.when((odd_x == px) & (odd_y == py))
            def _():
                low, top = (yb, ya) if py == 0 else (ya, yb)
                corners(low, top, out_a, px == 0)
                corners(low, top, out_b, px == 1)


def lanes(blocks):
    return jnp.concatenate(blocks, axis=1)


def own_lists(get, groups):
    left = lax.broadcasted_iota(I32, (16, 128), 1) < SLOTS
    first, last = [], []
    for i in range(groups // 2):
        a, b = get(2 * i), get(2 * i + 1)
        first.append(jnp.where(left, a, pltpu.roll(b, SLOTS, 1)))
        last.append(jnp.where(left, pltpu.roll(a, SLOTS, 1), b))
    return lanes(first), lanes(last)


def one_hot(code, count):
    width = code.shape[1]
    return (lax.broadcasted_iota(I32, (count, width), 0) == code).astype(F32).astype(BF16)


NT = (((1,), (1,)), ((), ()))


def place(parts, values, levels):
    a = [p * values[r + c : r + c + 1, :] for p, r in parts for c in range(6)]
    return lax.dot_general(jnp.concatenate(a, axis=0), levels, NT, preferred_element_type=F32)


def sided(groups, sides):
    plane = sides[12:13, :].astype(I32)
    level = sides[13:14, :].astype(I32)
    upper = lax.rem(lax.broadcasted_iota(I32, plane.shape, 1), 128) >= SLOTS
    x, y = plane // N, plane % N
    row = jnp.where(upper, y, y - 8)
    row = jnp.where(upper, jnp.where(y <= 5, row, -9999), jnp.where(y >= 10, row, -9999))
    levels = one_hot(jnp.where(upper, level + Z, level), 2 * Z)
    return x, row, levels


def place_own(lists, out_own, out_side):
    groups = lists.shape[0]
    first, last = own_lists(lambda g: lists[g, 16:32, :].astype(F32), groups)
    planes = one_hot(first[12:13, :].astype(I32), N * N)
    levels = one_hot(first[13:14, :].astype(I32), Z)
    first, last = first.astype(BF16), last.astype(BF16)
    for t in range(3):
        vals, row = (first, 6 * t) if t < 2 else (last, 0)
        spread = [levels * vals[row + c : row + c + 1, :] for c in range(6)]
        got = lax.dot_general(planes, jnp.concatenate(spread, axis=0), NT, preferred_element_type=F32)
        for c in range(6):
            out_own[6 * t + c] = got[:, Z * c : Z * c + Z]
    sides = lanes([lists[g, 0:16, :].astype(F32) for g in range(groups)])
    x, row, levels = sided(groups, sides)
    planes = one_hot(x * 8 + row, 8 * N)
    sides = sides.astype(BF16)
    got = place(((planes, 0), (planes, 6)), sides, levels)
    for k in range(12):
        out_side[k] = got[8 * N * k : 8 * N * k + 8 * N]


def roll_z(f, k, lane):
    moved = pltpu.roll(f, (-k) % Z, f.ndim - 1)
    keep = (lane < Z - k) if k > 0 else (lane >= -k)
    return jnp.where(keep, moved, 0.0)


def advance(xa, xb, ca, cb, ya, yb, v, s, mats, own, side, vout, sout, ev, es, eb, el, em, beyond, corner):
    odd_x = lax.rem(lax.axis_index("gx"), 2)
    odd_y = lax.rem(lax.axis_index("gy"), 2)
    refs = (v, s, mats.at[0], mats.at[1], mats.at[2])
    ext = (ev, es, eb, el, em)

    def at(x, y):
        return x * YE + y

    for q in range(NQ):
        src, dst = part(refs, q), part(ext, q)
        for x in range(N):
            dst[at(XO + x, YO) : at(XO + x, YO) + N, :] = src[N * x : N * x + N, :]

    def layer(msg, q, d):
        rows = msg[FACE_AT[q, d]].astype(F32)
        if d == 1:
            rows = rows + msg[LOW_AT[q]].astype(F32)
        return rows

    def put_y(low, top):
        for q in range(NQ):
            dst = part(ext, q)
            for d in range(1, DEPTH[q] + 1):
                dst[pl.ds(at(XO, YO - d), N, stride=YE), :] = layer(low, q, d)
                dst[pl.ds(at(XO, YO + N - 1 + d), N, stride=YE), :] = layer(top, q, d)

    def put_x(low, top):
        for q in range(NQ):
            dst = part(ext, q)
            for d in range(1, DEPTH[q] + 1):
                for msg, x in ((low, XO - d), (top, XO + N - 1 + d)):
                    dst[at(x, YO) : at(x, YO) + N, :] = layer(msg, q, d)

    def put_corners(low, top):
        for i, (q, d, far, m) in enumerate(CORN):
            dst = part(ext, q)
            for msg, x, back in ((low, XO - 8, 8 - m), (top, XO + N, m)):
                both = msg[i].astype(F32)
                for h in range(2):
                    rows = both[8 * h : 8 * h + 8]

                    def put(depth, rows):
                        y = YO + N - 1 + depth if h else YO - depth
                        dst[pl.ds(at(x, y), 8, stride=YE), :] = rows

                    put(d, rows)
                    if far:
                        put(far, pltpu.roll(rows, back, 0))

    for odd, put, one, two in ((odd_y, put_y, ya, yb), (odd_x, put_x, xa, xb), (odd_x, put_corners, ca, cb)):

        @pl.when(odd == 0)
        def _():
            put(two, one)

        @pl.when(odd == 1)
        def _():
            put(one, two)

    def total(terms):
        near = far = None
        for g, fwd in terms:
            k = 0 if fwd else -1
            p, q = g(1 + k) - g(k), g(2 + k) - g(k - 1)
            near, far = (p, q) if near is None else (near + p, far + q)
        return INNER * near + OUTER * far

    def reader(ref, x, y0, n):
        base = pl.multiple_of(x * YE, 8)

        def along_x(c):
            return lambda k: ref[c, pl.ds(base + (k * YE + y0), n), :]

        def along_y(c):
            return lambda k: ref[c, pl.ds(base + (y0 + k), n), :]

        def along_z(c):
            f = ref[c, pl.ds(base + y0, n), :]
            lane = lax.broadcasted_iota(I32, (n, Z), 1)
            return lambda k: f if k == 0 else roll_z(f, k, lane)

        return along_x, along_y, along_z, pl.ds(base + y0, n)

    def velocity_at(x, y0, n):
        ax, ay, az, here = reader(es, x, y0, n)
        buoy = eb[here, :]
        forces = (
            total(((ax(0), True), (ay(3), False), (az(4), False))),
            total(((ax(3), False), (ay(1), True), (az(5), False))),
            total(((ax(4), False), (ay(5), False), (az(2), True))),
        )
        for c, f in enumerate(forces):
            ev[c, here, :] = ev[c, here, :] + buoy * f

    def stress_at(x, y0, n):
        ax, ay, az, here = reader(ev, x, y0, n)
        lam, rig = el[here, :], em[here, :]
        d1, d2, d3 = total(((ax(0), False),)), total(((ay(1), False),)), total(((az(2), False),))
        e = lam * (d1 + d2 + d3)
        two = 2.0 * rig
        rates = (
            e + two * d1,
            e + two * d2,
            e + two * d3,
            rig * total(((ay(0), True), (ax(1), True))),
            rig * total(((az(0), True), (ax(2), True))),
            rig * total(((az(1), True), (ay(2), True))),
        )
        for c, r in enumerate(rates):
            es[c, here, :] = es[c, here, :] + r

    def sweep(fn, reach, y0, n):
        def step(x, carry):
            fn(x, y0, n)
            return carry

        lax.fori_loop(XO - reach, XO + N + reach, step, 0, unroll=UNROLL[reach])

    def add(c, x, y, rows):
        here = slice(at(x, y), at(x, y) + rows.shape[0])
        es[c, here, :] = es[c, here, :] + rows

    def add_own(t):
        for c in range(6):
            for x in range(N):
                add(c, XO + x, YO, own[6 * t + c, N * x : N * x + N, :])

    def add_side(t):
        for c in range(6):
            for x in range(N):
                rows = slice(8 * x, 8 * x + 8)
                add(c, XO + x, YO - 8, side[6 * t + c, rows, 0:Z])
                add(c, XO + x, YO + N, side[6 * t + c, rows, Z : 2 * Z])

    def place_beyond():
        groups = (ca.shape[0] - NCORN) // 2
        base = NCORN

        def one(msg, up, k):
            first, _ = own_lists(lambda g: msg[base + 2 * g + 1].astype(F32), groups)
            plane = first[12:13, :].astype(I32)
            levels = one_hot(first[13:14, :].astype(I32), Z)
            x, y = plane // N, plane % N

            def faces(far):
                i = x if up else x - (N - far)
                return one_hot(jnp.where(i >= 0, i * N + y, -1), far * N)

            parts = ((faces(FAR[0]), 0), (faces(FAR[1]), 6))
            beyond[k] = place(parts, first.astype(BF16), levels)
            sides = lanes([msg[base + 2 * g].astype(F32) for g in range(groups)])
            sx, row, levels = sided(groups, sides)

            def edges(near):
                i = sx if up else sx - (N - near)
                return one_hot(jnp.where(i >= 0, i * 8 + row, -1), 8 * near)

            parts = ((edges(NEAR[0]), 0), (edges(NEAR[1]), 6))
            corner[k] = place(parts, sides.astype(BF16), levels)

        @pl.when(odd_x == 0)
        def _():
            one(cb, False, 0)
            one(ca, True, 1)

        @pl.when(odd_x == 1)
        def _():
            one(ca, False, 0)
            one(cb, True, 1)

    def add_beyond(t):
        far, near = FAR[t], NEAR[t]
        f0, n0 = (0, 0) if t == 0 else (6 * N * FAR[0], 6 * 8 * NEAR[0])
        for k in range(2):
            for c in range(6):
                x0 = XO + N if k else XO - far
                for i in range(far):
                    r = f0 + N * (c * far + i)
                    add(c, x0 + i, YO, beyond[k, r : r + N, :])
                x0 = XO + N if k else XO - near
                for i in range(near):
                    r = n0 + 8 * (c * near + i)
                    add(c, x0 + i, YO - 8, corner[k, r : r + 8, 0:Z])
                    add(c, x0 + i, YO + N, corner[k, r : r + 8, Z : 2 * Z])

    place_beyond()
    sweep(velocity_at, 8, 8, 32)
    sweep(stress_at, 6, 8, 32)
    add_own(0)
    add_side(0)
    add_beyond(0)
    sweep(velocity_at, 5, 8, 32)
    sweep(stress_at, 3, 13, 24)
    add_own(1)
    add_side(1)
    add_beyond(1)
    sweep(velocity_at, 2, 14, 24)
    sweep(stress_at, 0, 16, 16)
    for x in range(N):
        here = slice(at(XO + x, YO), at(XO + x, YO) + N)
        rows = slice(N * x, N * x + N)
        for c in range(3):
            vout[c, rows, :] = ev[c, here, :]
        for c in range(6):
            sout[c, rows, :] = es[c, here, :] + own[12 + c, rows, :]


SCRATCH = [pltpu.VMEM((n, XE * YE, Z), F32) for n in (3, 6)] + [pltpu.VMEM((XE * YE, Z), F32)] * 3
SCRATCH += [
    pltpu.VMEM((2, 6 * N * (FAR[0] + FAR[1]), Z), F32),
    pltpu.VMEM((2, 6 * 8 * (NEAR[0] + NEAR[1]), 2 * Z), F32),
]


def swaps(count, first):
    pairs = []
    for i in range(first, count - 1, 2):
        pairs += [(i, i + 1), (i + 1, i)]
    return pairs


def swap_both(a, b, axis):
    count = lax.axis_size(axis)
    return (
        lax.ppermute(a, axis, swaps(count, 0)),
        lax.ppermute(b, axis, swaps(count, 1)),
    )


def call(kernel, outs, args, scratch=(), flops=1_000_000, mib=8, here=True):
    if not here:
        held = [pltpu.VMEM(a.shape, a.dtype) for a in args]
        scratch = held + list(scratch) + [pltpu.SemaphoreType.DMA((len(args),))]
    return pl.pallas_call(
        kernel,
        out_shape=[jax.ShapeDtypeStruct(s, t) for s, t in outs],
        in_specs=[vmem() if here else pl.BlockSpec(memory_space=pltpu.HBM)] * len(args),
        out_specs=[vmem()] * len(outs),
        scratch_shapes=list(scratch),
        compiler_params=pltpu.CompilerParams(vmem_limit_bytes=mib * 1024 * 1024),
        cost_estimate=pl.CostEstimate(flops=flops, bytes_accessed=1_000_000, transcendentals=0),
    )(*args)


def local(velocity, stresses, buoyancy, lame, rigidity, hist, mech, res, owners, cells):
    groups = lax.axis_size("gy")
    v = velocity.reshape(3, N * N, Z)
    s = stresses.reshape(6, N * N, Z)
    b, l, m = (a.reshape(N * N, Z) for a in (buoyancy, lame, rigidity))
    state = (v, s, b, l, m)
    mats = jnp.stack([b, l, m])
    later = (v, s, mats)
    face = ((NFACE, N, Z), BF16)
    rows = hist.shape[0]
    ya, yb, sent = call(
        lambda *refs: opening(groups, *refs),
        [face, face, ((groups, 32, 128), BF16)],
        state + (hist, mech.T, res.T, owners.reshape(1, rows), cells.reshape(1, rows)),
        [pltpu.VMEM((32, rows), F32)],
        here=False,
        mib=FIRST,
    )
    ya, yb = swap_both(ya, yb, "gy")
    lists = lax.all_to_all(sent, "gy", split_axis=0, concat_axis=0, tiled=True)
    xa, xb = call(pack_x, [face, face], later)
    xa, xb = swap_both(xa, xb, "gx")
    rest = ((NCORN + 2 * groups, N, Z), BF16)
    ca, cb = call(pack_corners, [rest, rest], (ya, yb, lists))
    ca, cb = swap_both(ca, cb, "gx")
    own, side = call(
        place_own,
        [((18, N * N, Z), F32), ((12, 8 * N, 2 * Z), F32)],
        (lists,),
        flops=10_000_000_000,
        mib=24,
    )
    vout, sout = call(
        advance,
        [(v.shape, F32), (s.shape, F32)],
        (xa, xb, ca, cb, ya, yb) + later + (own, side),
        SCRATCH,
        mib=24,
    )
    return vout.reshape(velocity.shape), sout.reshape(stresses.shape)


def solution(mesh):
    in_specs = (
        P(None, "gx", "gy", None),
        P(None, "gx", "gy", None),
        P("gx", "gy", None),
        P("gx", "gy", None),
        P("gx", "gy", None),
        P(("gx", "gy"), None),
        P(("gx", "gy"), None),
        P(),
        P(("gx", "gy"), None),
        P(("gx", "gy")),
    )
    out_specs = (P(None, "gx", "gy", None), P(None, "gx", "gy", None))
    return jax.shard_map(local, mesh=mesh, in_specs=in_specs, out_specs=out_specs, check_vma=False)
```

```python
import jax
import jax.numpy as jnp
from jax import lax
from jax.experimental import pallas as pl
from jax.experimental.pallas import tpu as pltpu
from jax.sharding import PartitionSpec as P

INNER = 9.0 / 8.0
OUTER = -1.0 / 24.0
F32, BF16, I32 = jnp.float32, jnp.bfloat16, jnp.int32

N = 16
Z = 128
XO = 11
XE = XO + N + 10
YO = 16
YE = 40
DEPTH = [9] * 6 + [8] * 3 + [8, 6, 6]
CORNER = [8] * 6 + [6] * 3 + [6, 5, 5]
NQ = len(DEPTH)
FACE = [(q, d) for q in range(NQ) for d in range(1, DEPTH[q] + 1)]
FACE_AT = {qd: i for i, qd in enumerate(FACE)}
LOW_AT = {q: len(FACE) + q for q in range(NQ)}
NFACE = len(FACE) + NQ
PACKED = {
    8: ((1, 0, 0), (2, 0, 0), (3, 7, 2), (4, 6, 3), (5, 8, 2)),
    6: ((1, 6, 2), (2, 0, 0), (3, 4, 3), (5, 0, 0)),
    5: ((1, 3, 3), (2, 4, 2), (5, 0, 0)),
}
CORN = [(q,) + unit for q in range(NQ) for unit in PACKED[CORNER[q]]]
NCORN = len(CORN)
SLOTS = 64
FAR = (6, 3)
NEAR = (5, 2)


def vmem():
    return pl.BlockSpec(memory_space=pltpu.VMEM)


def part(refs, q):
    v, s, b, l, m = refs
    if q < 6:
        return s.at[q]
    if q < 9:
        return v.at[q - 6]
    return (b, l, m)[q - 9]


def split(x):
    hi = x.astype(BF16)
    return hi, (x - hi.astype(F32)).astype(BF16)


def fetch(pairs, sems):
    copies = [pltpu.make_async_copy(a, b, sems.at[i]) for i, (a, b) in enumerate(pairs)]
    for copy in copies:
        copy.start()
    return copies


def opening(groups, *refs):
    given, (out_a, out_b, sent, mats), held, vals, sems = refs[:10], refs[10:14], refs[14:24], refs[24], refs[25]
    copies = fetch(list(zip(given, held)), sems)
    for copy in copies[5:]:
        copy.wait()
    route(groups, *held[5:], sent, vals)
    for copy in copies[:5]:
        copy.wait()
    pack_y(*held[:5], out_a, out_b)
    for i in range(3):
        mats[i] = held[2 + i][...]


def pack_y(v, s, b, l, m, out_a, out_b):
    odd = lax.rem(lax.axis_index("gy"), 2)
    refs = (v, s, b, l, m)
    for out, high in ((out_a, odd == 0), (out_b, odd == 1)):
        for q in range(NQ):
            src = part(refs, q)
            for d in range(1, DEPTH[q] + 1):
                y = jnp.where(high, N - d, d - 1)
                rows = src[pl.ds(y, N, stride=N), :]
                if d == 1:
                    hi, lo = split(rows)
                    out[FACE_AT[q, d]] = hi
                    out[LOW_AT[q]] = lo
                else:
                    out[FACE_AT[q, d]] = rows.astype(BF16)


def route(groups, hist, mech, res, owners, cells, out, vals):
    rows = hist.shape[0]
    nt = (((1,), (1,)), ((), ()))
    amp = lax.dot_general(res[...], hist[...], nt, preferred_element_type=F32)
    mechf = mech[...].astype(F32)
    vals[...] = jnp.zeros_like(vals)
    vals[0:6] = mechf * amp[0:1]
    vals[6:12] = mechf * amp[1:2]
    vals[16:22] = mechf * amp[2:3]
    cell = cells[...]
    vals[12:13] = (cell // Z).astype(F32)
    vals[13:14] = (cell % Z).astype(F32)
    v = vals[...].astype(BF16)
    own = owners[...]
    hits = (lax.broadcasted_iota(I32, (groups, rows), 0) == own).astype(F32)
    r0 = lax.broadcasted_iota(I32, (rows, rows), 0)
    r1 = lax.broadcasted_iota(I32, (rows, rows), 1)
    before = (r0 < r1).astype(F32).astype(BF16)
    earlier = jnp.dot(hits.astype(BF16), before, preferred_element_type=F32)
    rank = jnp.sum(hits * earlier, axis=0, keepdims=True)
    slot = own * SLOTS + rank.astype(I32)
    total = groups * SLOTS
    pick = (lax.broadcasted_iota(I32, (total, rows), 0) == slot).astype(F32).astype(BF16)
    sent = lax.dot_general(v, pick, nt, preferred_element_type=F32)
    turned = pltpu.roll(sent, SLOTS, 1)
    left = lax.broadcasted_iota(I32, (16, 2 * SLOTS), 1) < SLOTS
    zero = jnp.zeros((16, 2 * SLOTS), F32)

    def plain(j, h):
        return sent[16 * h : 16 * h + 16, 128 * j : 128 * j + 128]

    def shifted(j, h):
        j = j % (groups // 2)
        return turned[16 * h : 16 * h + 16, 128 * j : 128 * j + 128]

    for o in range(groups):
        j = o // 2
        if o % 2 == 0:
            sides = jnp.where(left, shifted(j, 0) if j else zero, plain(j, 0))
            mine = jnp.where(left, plain(j, 0), shifted(j, 1))
        else:
            last = o == groups - 1
            sides = jnp.where(left, plain(j, 0), zero if last else shifted(j + 1, 0))
            mine = jnp.where(left, shifted(j + 1, 0), plain(j, 1))
        out[o, 0:16, :] = sides.astype(BF16)
        out[o, 16:32, :] = mine.astype(BF16)


def pack_x(v, s, mats, out_a, out_b):
    odd = lax.rem(lax.axis_index("gx"), 2)
    refs = (v, s, mats.at[0], mats.at[1], mats.at[2])
    for out, high in ((out_a, odd == 0), (out_b, odd == 1)):
        for q in range(NQ):
            src = part(refs, q)
            for d in range(1, DEPTH[q] + 1):
                x = jnp.where(high, N - d, d - 1)
                rows = src[pl.ds(pl.multiple_of(x * N, N), N), :]
                if d == 1:
                    hi, lo = split(rows)
                    out[FACE_AT[q, d]] = hi
                    out[LOW_AT[q]] = lo
                else:
                    out[FACE_AT[q, d]] = rows.astype(BF16)


def pack_corners(ya, yb, lists, out_a, out_b):
    odd_x = lax.rem(lax.axis_index("gx"), 2)
    odd_y = lax.rem(lax.axis_index("gy"), 2)
    groups = lists.shape[0]
    first, _ = own_lists(lambda g: lists[g, 16:32, :].astype(F32), groups)
    first = first.astype(BF16)
    for out in (out_a, out_b):
        for g in range(groups):
            out[NCORN + g] = lists[g, 0:16, :]
        for g in range(groups // 2):
            out[NCORN + groups + g] = first[:, 128 * g : 128 * g + 128]

    def corners(low, top, out, high):
        row = lax.broadcasted_iota(I32, (8, Z), 0)
        k = 8 if high else 0
        for i, (q, d, far, m) in enumerate(CORN):
            halves = []
            for msg in (low, top):
                a = msg[FACE_AT[q, d]].astype(F32)[k : k + 8]
                if far:
                    c = msg[FACE_AT[q, far]].astype(F32)[k : k + 8]
                    if high:
                        a = jnp.where(row < m, pltpu.roll(c, m, 0), a)
                    else:
                        a = jnp.where(row >= 8 - m, pltpu.roll(c, 8 - m, 0), a)
                halves.append(a)
            out[i] = jnp.concatenate(halves, axis=0).astype(BF16)

    for px in range(2):
        for py in range(2):

            @pl.when((odd_x == px) & (odd_y == py))
            def _():
                low, top = (yb, ya) if py == 0 else (ya, yb)
                corners(low, top, out_a, px == 0)
                corners(low, top, out_b, px == 1)


def lanes(blocks):
    return jnp.concatenate(blocks, axis=1)


def own_lists(get, groups):
    left = lax.broadcasted_iota(I32, (16, 128), 1) < SLOTS
    first, last = [], []
    for i in range(groups // 2):
        a, b = get(2 * i), get(2 * i + 1)
        first.append(jnp.where(left, a, pltpu.roll(b, SLOTS, 1)))
        last.append(jnp.where(left, pltpu.roll(a, SLOTS, 1), b))
    return lanes(first), lanes(last)


def one_hot(code, count):
    width = code.shape[1]
    return (lax.broadcasted_iota(I32, (count, width), 0) == code).astype(F32).astype(BF16)


NT = (((1,), (1,)), ((), ()))


def place(parts, values, levels):
    a = [p * values[r + c : r + c + 1, :] for p, r in parts for c in range(6)]
    return lax.dot_general(jnp.concatenate(a, axis=0), levels, NT, preferred_element_type=F32)


def sided(groups, sides):
    plane = sides[12:13, :].astype(I32)
    level = sides[13:14, :].astype(I32)
    upper = lax.rem(lax.broadcasted_iota(I32, plane.shape, 1), 128) >= SLOTS
    x, y = plane // N, plane % N
    row = jnp.where(upper, y, y - 8)
    row = jnp.where(upper, jnp.where(y <= 5, row, -9999), jnp.where(y >= 10, row, -9999))
    levels = one_hot(jnp.where(upper, level + Z, level), 2 * Z)
    return x, row, levels


def place_own(lists, out_own, out_side):
    groups = lists.shape[0]
    first, last = own_lists(lambda g: lists[g, 16:32, :].astype(F32), groups)
    planes = one_hot(first[12:13, :].astype(I32), N * N)
    levels = one_hot(first[13:14, :].astype(I32), Z)
    first, last = first.astype(BF16), last.astype(BF16)
    for t in range(3):
        vals, row = (first, 6 * t) if t < 2 else (last, 0)
        spread = [levels * vals[row + c : row + c + 1, :] for c in range(6)]
        got = lax.dot_general(planes, jnp.concatenate(spread, axis=0), NT, preferred_element_type=F32)
        for c in range(6):
            out_own[6 * t + c] = got[:, Z * c : Z * c + Z]
    sides = lanes([lists[g, 0:16, :].astype(F32) for g in range(groups)])
    x, row, levels = sided(groups, sides)
    planes = one_hot(x * 8 + row, 8 * N)
    sides = sides.astype(BF16)
    got = place(((planes, 0), (planes, 6)), sides, levels)
    for k in range(12):
        out_side[k] = got[8 * N * k : 8 * N * k + 8 * N]


def roll_z(f, k, lane):
    moved = pltpu.roll(f, (-k) % Z, f.ndim - 1)
    keep = (lane < Z - k) if k > 0 else (lane >= -k)
    return jnp.where(keep, moved, 0.0)


def advance(xa, xb, ca, cb, ya, yb, v, s, mats, own, side, vout, sout, ev, es, eb, el, em, beyond, corner):
    odd_x = lax.rem(lax.axis_index("gx"), 2)
    odd_y = lax.rem(lax.axis_index("gy"), 2)
    refs = (v, s, mats.at[0], mats.at[1], mats.at[2])
    ext = (ev, es, eb, el, em)

    def at(x, y):
        return x * YE + y

    for q in range(NQ):
        src, dst = part(refs, q), part(ext, q)
        for x in range(N):
            dst[at(XO + x, YO) : at(XO + x, YO) + N, :] = src[N * x : N * x + N, :]

    def layer(msg, q, d):
        rows = msg[FACE_AT[q, d]].astype(F32)
        if d == 1:
            rows = rows + msg[LOW_AT[q]].astype(F32)
        return rows

    def put_y(low, top):
        for q in range(NQ):
            dst = part(ext, q)
            for d in range(1, DEPTH[q] + 1):
                dst[pl.ds(at(XO, YO - d), N, stride=YE), :] = layer(low, q, d)
                dst[pl.ds(at(XO, YO + N - 1 + d), N, stride=YE), :] = layer(top, q, d)

    def put_x(low, top):
        for q in range(NQ):
            dst = part(ext, q)
            for d in range(1, DEPTH[q] + 1):
                for msg, x in ((low, XO - d), (top, XO + N - 1 + d)):
                    dst[at(x, YO) : at(x, YO) + N, :] = layer(msg, q, d)

    def put_corners(low, top):
        for i, (q, d, far, m) in enumerate(CORN):
            dst = part(ext, q)
            for msg, x, back in ((low, XO - 8, 8 - m), (top, XO + N, m)):
                both = msg[i].astype(F32)
                for h in range(2):
                    rows = both[8 * h : 8 * h + 8]

                    def put(depth, rows):
                        y = YO + N - 1 + depth if h else YO - depth
                        dst[pl.ds(at(x, y), 8, stride=YE), :] = rows

                    put(d, rows)
                    if far:
                        put(far, pltpu.roll(rows, back, 0))

    for odd, put, one, two in ((odd_y, put_y, ya, yb), (odd_x, put_x, xa, xb), (odd_x, put_corners, ca, cb)):

        @pl.when(odd == 0)
        def _():
            put(two, one)

        @pl.when(odd == 1)
        def _():
            put(one, two)

    def total(terms):
        near = far = None
        for g, fwd in terms:
            k = 0 if fwd else -1
            p, q = g(1 + k) - g(k), g(2 + k) - g(k - 1)
            near, far = (p, q) if near is None else (near + p, far + q)
        return INNER * near + OUTER * far

    def reader(ref, x, y0, n):
        base = x * YE if isinstance(x, int) else pl.multiple_of(x * YE, 8)

        def along_x(c):
            return lambda k: ref[c, pl.ds(base + (k * YE + y0), n), :]

        def along_y(c):
            return lambda k: ref[c, pl.ds(base + (y0 + k), n), :]

        def along_z(c):
            f = ref[c, pl.ds(base + y0, n), :]
            lane = lax.broadcasted_iota(I32, (n, Z), 1)
            return lambda k: f if k == 0 else roll_z(f, k, lane)

        return along_x, along_y, along_z, pl.ds(base + y0, n)

    def velocity_at(x, y0, n):
        ax, ay, az, here = reader(es, x, y0, n)
        buoy = eb[here, :]
        forces = (
            total(((ax(0), True), (ay(3), False), (az(4), False))),
            total(((ax(3), False), (ay(1), True), (az(5), False))),
            total(((ax(4), False), (ay(5), False), (az(2), True))),
        )
        for c, f in enumerate(forces):
            ev[c, here, :] = ev[c, here, :] + buoy * f

    def stress_at(x, y0, n):
        ax, ay, az, here = reader(ev, x, y0, n)
        lam, rig = el[here, :], em[here, :]
        d1, d2, d3 = total(((ax(0), False),)), total(((ay(1), False),)), total(((az(2), False),))
        e = lam * (d1 + d2 + d3)
        two = 2.0 * rig
        rates = (
            e + two * d1,
            e + two * d2,
            e + two * d3,
            rig * total(((ay(0), True), (ax(1), True))),
            rig * total(((az(0), True), (ax(2), True))),
            rig * total(((az(1), True), (ay(2), True))),
        )
        for c, r in enumerate(rates):
            es[c, here, :] = es[c, here, :] + r

    def sweep(fn, wide, y0, n, sides, unroll):
        def step(x, carry):
            fn(x, y0, n)
            return carry

        lax.fori_loop(XO - wide, XO + N + wide, step, 0, unroll=unroll)
        for depth, rows in sides:
            for x in (XO - depth, XO + N - 1 + depth):
                fn(x, YO + (N - rows) // 2, rows)

    def add(c, x, y, rows):
        here = slice(at(x, y), at(x, y) + rows.shape[0])
        es[c, here, :] = es[c, here, :] + rows

    def add_own(t):
        for c in range(6):
            for x in range(N):
                add(c, XO + x, YO, own[6 * t + c, N * x : N * x + N, :])

    def add_side(t):
        for c in range(6):
            for x in range(N):
                rows = slice(8 * x, 8 * x + 8)
                add(c, XO + x, YO - 8, side[6 * t + c, rows, 0:Z])
                add(c, XO + x, YO + N, side[6 * t + c, rows, Z : 2 * Z])

    def place_beyond():
        groups = (ca.shape[0] - NCORN) * 2 // 3
        base = NCORN

        def one(msg, up, k):
            first = lanes([msg[base + groups + g].astype(F32) for g in range(groups // 2)])
            plane = first[12:13, :].astype(I32)
            levels = one_hot(first[13:14, :].astype(I32), Z)
            x, y = plane // N, plane % N

            def faces(far):
                i = x if up else x - (N - far)
                return one_hot(jnp.where(i >= 0, i * N + y, -1), far * N)

            parts = ((faces(FAR[0]), 0), (faces(FAR[1]), 6))
            beyond[k] = place(parts, first.astype(BF16), levels)
            sides = lanes([msg[base + g].astype(F32) for g in range(groups)])
            sx, row, levels = sided(groups, sides)

            def edges(near):
                i = sx if up else sx - (N - near)
                return one_hot(jnp.where(i >= 0, i * 8 + row, -1), 8 * near)

            parts = ((edges(NEAR[0]), 0), (edges(NEAR[1]), 6))
            corner[k] = place(parts, sides.astype(BF16), levels)

        @pl.when(odd_x == 0)
        def _():
            one(cb, False, 0)
            one(ca, True, 1)

        @pl.when(odd_x == 1)
        def _():
            one(ca, False, 0)
            one(cb, True, 1)

    def add_beyond(t):
        far, near = FAR[t], NEAR[t]
        f0, n0 = (0, 0) if t == 0 else (6 * N * FAR[0], 6 * 8 * NEAR[0])
        for k in range(2):
            for c in range(6):
                x0 = XO + N if k else XO - far
                for i in range(far):
                    r = f0 + N * (c * far + i)
                    add(c, x0 + i, YO, beyond[k, r : r + N, :])
                x0 = XO + N if k else XO - near
                for i in range(near):
                    r = n0 + 8 * (c * near + i)
                    add(c, x0 + i, YO - 8, corner[k, r : r + 8, 0:Z])
                    add(c, x0 + i, YO + N, corner[k, r : r + 8, Z : 2 * Z])

    place_beyond()
    sweep(velocity_at, 4, 8, 32, ((5, 24), (6, 24), (7, 16), (8, 16)), 8)
    sweep(stress_at, 2, 8, 32, ((3, 24), (4, 24), (5, 24), (6, 16)), 10)
    add_own(0)
    add_side(0)
    add_beyond(0)
    sweep(velocity_at, 0, 8, 32, ((1, 24), (2, 24), (3, 24), (4, 16), (5, 16)), 8)
    sweep(stress_at, 2, 12, 24, ((3, 16),), 10)
    add_own(1)
    add_side(1)
    add_beyond(1)
    sweep(velocity_at, 0, 12, 24, ((1, 16), (2, 16)), 8)
    sweep(stress_at, 0, 16, 16, (), 8)
    for x in range(N):
        here = slice(at(XO + x, YO), at(XO + x, YO) + N)
        rows = slice(N * x, N * x + N)
        for c in range(3):
            vout[c, rows, :] = ev[c, here, :]
        for c in range(6):
            sout[c, rows, :] = es[c, here, :] + own[12 + c, rows, :]


SCRATCH = [pltpu.VMEM((n, XE * YE, Z), F32) for n in (3, 6)] + [pltpu.VMEM((XE * YE, Z), F32)] * 3
SCRATCH += [
    pltpu.VMEM((2, 6 * N * (FAR[0] + FAR[1]), Z), F32),
    pltpu.VMEM((2, 6 * 8 * (NEAR[0] + NEAR[1]), 2 * Z), F32),
]


def swaps(count, first):
    pairs = []
    for i in range(first, count - 1, 2):
        pairs += [(i, i + 1), (i + 1, i)]
    return pairs


def swap_both(a, b, axis):
    count = lax.axis_size(axis)
    return (
        lax.ppermute(a, axis, swaps(count, 0)),
        lax.ppermute(b, axis, swaps(count, 1)),
    )


def call(kernel, outs, args, scratch=(), flops=1_000_000, mib=8, here=True, keep=True):
    if not here:
        held = [pltpu.VMEM(a.shape, a.dtype) for a in args]
        args = [pltpu.with_memory_space_constraint(a, pltpu.HBM) for a in args]
        scratch = held + list(scratch) + [pltpu.SemaphoreType.DMA((len(args),))]
    return pl.pallas_call(
        kernel,
        out_shape=[(pltpu.VMEM if keep else jax.ShapeDtypeStruct)(s, t) for s, t in outs],
        in_specs=[vmem() if here else pl.BlockSpec(memory_space=pltpu.HBM)] * len(args),
        out_specs=[vmem()] * len(outs),
        scratch_shapes=list(scratch),
        compiler_params=pltpu.CompilerParams(vmem_limit_bytes=mib * 1024 * 1024),
        cost_estimate=pl.CostEstimate(flops=flops, bytes_accessed=1_000_000, transcendentals=0),
    )(*args)


def local(velocity, stresses, buoyancy, lame, rigidity, hist, mech, res, owners, cells):
    groups = lax.axis_size("gy")
    v = velocity.reshape(3, N * N, Z)
    s = stresses.reshape(6, N * N, Z)
    b, l, m = (a.reshape(N * N, Z) for a in (buoyancy, lame, rigidity))
    state = (v, s, b, l, m)
    face = ((NFACE, N, Z), BF16)
    rows = hist.shape[0]
    ya, yb, sent, mats = call(
        lambda *refs: opening(groups, *refs),
        [face, face, ((groups, 32, 128), BF16), ((3, N * N, Z), F32)],
        state + (hist, mech.T, res.T, owners.reshape(1, rows), cells.reshape(1, rows)),
        [pltpu.VMEM((32, rows), F32)],
        here=False,
    )
    later = (v, s, mats)
    ya, yb = swap_both(ya, yb, "gy")
    lists = lax.all_to_all(sent, "gy", split_axis=0, concat_axis=0, tiled=True)
    xa, xb = call(pack_x, [face, face], later)
    xa, xb = swap_both(xa, xb, "gx")
    rest = ((NCORN + groups + groups // 2, N, Z), BF16)
    ca, cb = call(pack_corners, [rest, rest], (ya, yb, lists))
    ca, cb = swap_both(ca, cb, "gx")
    own, side = call(
        place_own,
        [((18, N * N, Z), F32), ((12, 8 * N, 2 * Z), F32)],
        (lists,),
        flops=10_000_000_000,
        mib=24,
    )
    vout, sout = call(
        advance,
        [(v.shape, F32), (s.shape, F32)],
        (xa, xb, ca, cb, ya, yb) + later + (own, side),
        SCRATCH,
        keep=False,
        mib=24,
    )
    return vout.reshape(velocity.shape), sout.reshape(stresses.shape)


def solution(mesh):
    in_specs = (
        P(None, "gx", "gy", None),
        P(None, "gx", "gy", None),
        P("gx", "gy", None),
        P("gx", "gy", None),
        P("gx", "gy", None),
        P(("gx", "gy"), None),
        P(("gx", "gy"), None),
        P(),
        P(("gx", "gy"), None),
        P(("gx", "gy")),
    )
    out_specs = (P(None, "gx", "gy", None), P(None, "gx", "gy", None))
    return jax.shard_map(local, mesh=mesh, in_specs=in_specs, out_specs=out_specs, check_vma=False)
```

```python
import jax
import jax.numpy as jnp
from jax import lax
from jax.experimental import pallas as pl
from jax.experimental.pallas import tpu as pltpu
from jax.sharding import PartitionSpec as P

INNER = 9.0 / 8.0
OUTER = -1.0 / 24.0
F32, BF16, I32 = jnp.float32, jnp.bfloat16, jnp.int32

N = 16
Z = 128
XO = 11
XE = XO + N + 10
YO = 16
YE = 40
DEPTH = [9] * 6 + [8] * 3 + [8, 6, 6]
CORNER = [8] * 6 + [6] * 3 + [6, 5, 5]
NQ = len(DEPTH)
FACE = [(q, d) for q in range(NQ) for d in range(1, DEPTH[q] + 1)]
FACE_AT = {qd: i for i, qd in enumerate(FACE)}
LOW_AT = {q: len(FACE) + q for q in range(NQ)}
NFACE = len(FACE) + NQ
PACKED = {
    8: ((1, 0, 0), (2, 0, 0), (3, 7, 2), (4, 6, 3), (5, 8, 2)),
    6: ((1, 6, 2), (2, 0, 0), (3, 4, 3), (5, 0, 0)),
    5: ((1, 3, 3), (2, 4, 2), (5, 0, 0)),
}
CORN = [(q,) + unit for q in range(NQ) for unit in PACKED[CORNER[q]]]
NCORN = len(CORN)
SLOTS = 64
LIMIT = (24, 24)
FAR = (6, 3)
NEAR = (5, 2)


def vmem():
    return pl.BlockSpec(memory_space=pltpu.VMEM)


def part(refs, q):
    v, s, b, l, m = refs
    if q < 6:
        return s.at[q]
    if q < 9:
        return v.at[q - 6]
    return (b, l, m)[q - 9]


def split(x):
    hi = x.astype(BF16)
    return hi, (x - hi.astype(F32)).astype(BF16)


def fetch(pairs, sems):
    copies = [pltpu.make_async_copy(a, b, sems.at[i]) for i, (a, b) in enumerate(pairs)]
    for copy in copies:
        copy.start()
    return copies


def opening(groups, *refs):
    given, (out_a, out_b, sent, mats), held, vals, sems = refs[:10], refs[10:14], refs[14:24], refs[24], refs[25]
    copies = fetch(list(zip(given, held)), sems)
    for copy in copies[5:]:
        copy.wait()
    route(groups, *held[5:], sent, vals)
    for copy in copies[:5]:
        copy.wait()
    pack_y(*held[:5], out_a, out_b)
    for i in range(3):
        mats[i] = held[2 + i][...]


def pack_y(v, s, b, l, m, out_a, out_b):
    odd = lax.rem(lax.axis_index("gy"), 2)
    refs = (v, s, b, l, m)
    for out, high in ((out_a, odd == 0), (out_b, odd == 1)):
        for q in range(NQ):
            src = part(refs, q)
            for d in range(1, DEPTH[q] + 1):
                y = jnp.where(high, N - d, d - 1)
                rows = src[pl.ds(y, N, stride=N), :]
                if d == 1:
                    hi, lo = split(rows)
                    out[FACE_AT[q, d]] = hi
                    out[LOW_AT[q]] = lo
                else:
                    out[FACE_AT[q, d]] = rows.astype(BF16)


def route(groups, hist, mech, res, owners, cells, out, vals):
    rows = hist.shape[0]
    nt = (((1,), (1,)), ((), ()))
    amp = lax.dot_general(res[...], hist[...], nt, preferred_element_type=F32)
    mechf = mech[...].astype(F32)
    vals[...] = jnp.zeros_like(vals)
    vals[0:6] = mechf * amp[0:1]
    vals[6:12] = mechf * amp[1:2]
    vals[16:22] = mechf * amp[2:3]
    cell = cells[...]
    vals[12:13] = (cell // Z).astype(F32)
    vals[13:14] = (cell % Z).astype(F32)
    v = vals[...].astype(BF16)
    own = owners[...]
    hits = (lax.broadcasted_iota(I32, (groups, rows), 0) == own).astype(F32)
    r0 = lax.broadcasted_iota(I32, (rows, rows), 0)
    r1 = lax.broadcasted_iota(I32, (rows, rows), 1)
    before = (r0 < r1).astype(F32).astype(BF16)
    earlier = jnp.dot(hits.astype(BF16), before, preferred_element_type=F32)
    rank = jnp.sum(hits * earlier, axis=0, keepdims=True)
    slot = own * SLOTS + rank.astype(I32)
    total = groups * SLOTS
    pick = (lax.broadcasted_iota(I32, (total, rows), 0) == slot).astype(F32).astype(BF16)
    sent = lax.dot_general(v, pick, nt, preferred_element_type=F32)
    turned = pltpu.roll(sent, SLOTS, 1)
    left = lax.broadcasted_iota(I32, (16, 2 * SLOTS), 1) < SLOTS
    zero = jnp.zeros((16, 2 * SLOTS), F32)

    def plain(j, h):
        return sent[16 * h : 16 * h + 16, 128 * j : 128 * j + 128]

    def shifted(j, h):
        j = j % (groups // 2)
        return turned[16 * h : 16 * h + 16, 128 * j : 128 * j + 128]

    for o in range(groups):
        j = o // 2
        if o % 2 == 0:
            sides = jnp.where(left, shifted(j, 0) if j else zero, plain(j, 0))
            mine = jnp.where(left, plain(j, 0), shifted(j, 1))
        else:
            last = o == groups - 1
            sides = jnp.where(left, plain(j, 0), zero if last else shifted(j + 1, 0))
            mine = jnp.where(left, shifted(j + 1, 0), plain(j, 1))
        out[o, 0:16, :] = sides.astype(BF16)
        out[o, 16:32, :] = mine.astype(BF16)


def pack_x(v, s, mats, out_a, out_b):
    odd = lax.rem(lax.axis_index("gx"), 2)
    refs = (v, s, mats.at[0], mats.at[1], mats.at[2])
    for out, high in ((out_a, odd == 0), (out_b, odd == 1)):
        for q in range(NQ):
            src = part(refs, q)
            for d in range(1, DEPTH[q] + 1):
                x = jnp.where(high, N - d, d - 1)
                rows = src[pl.ds(pl.multiple_of(x * N, N), N), :]
                if d == 1:
                    hi, lo = split(rows)
                    out[FACE_AT[q, d]] = hi
                    out[LOW_AT[q]] = lo
                else:
                    out[FACE_AT[q, d]] = rows.astype(BF16)


def pack_corners(ya, yb, lists, out_a, out_b):
    odd_x = lax.rem(lax.axis_index("gx"), 2)
    odd_y = lax.rem(lax.axis_index("gy"), 2)
    groups = lists.shape[0]
    first, _ = own_lists(lambda g: lists[g, 16:32, :].astype(F32), groups)
    first = first.astype(BF16)
    for out in (out_a, out_b):
        for g in range(groups):
            out[NCORN + g] = lists[g, 0:16, :]
        for g in range(groups // 2):
            out[NCORN + groups + g] = first[:, 128 * g : 128 * g + 128]

    def corners(low, top, out, high):
        row = lax.broadcasted_iota(I32, (8, Z), 0)
        k = 8 if high else 0
        for i, (q, d, far, m) in enumerate(CORN):
            halves = []
            for msg in (low, top):
                a = msg[FACE_AT[q, d]].astype(F32)[k : k + 8]
                if far:
                    c = msg[FACE_AT[q, far]].astype(F32)[k : k + 8]
                    if high:
                        a = jnp.where(row < m, pltpu.roll(c, m, 0), a)
                    else:
                        a = jnp.where(row >= 8 - m, pltpu.roll(c, 8 - m, 0), a)
                halves.append(a)
            out[i] = jnp.concatenate(halves, axis=0).astype(BF16)

    for px in range(2):
        for py in range(2):

            @pl.when((odd_x == px) & (odd_y == py))
            def _():
                low, top = (yb, ya) if py == 0 else (ya, yb)
                corners(low, top, out_a, px == 0)
                corners(low, top, out_b, px == 1)


def lanes(blocks):
    return jnp.concatenate(blocks, axis=1)


def own_lists(get, groups):
    left = lax.broadcasted_iota(I32, (16, 128), 1) < SLOTS
    first, last = [], []
    for i in range(groups // 2):
        a, b = get(2 * i), get(2 * i + 1)
        first.append(jnp.where(left, a, pltpu.roll(b, SLOTS, 1)))
        last.append(jnp.where(left, pltpu.roll(a, SLOTS, 1), b))
    return lanes(first), lanes(last)


def one_hot(code, count):
    width = code.shape[1]
    return (lax.broadcasted_iota(I32, (count, width), 0) == code).astype(F32).astype(BF16)


NT = (((1,), (1,)), ((), ()))


def place(parts, values, levels):
    a = [p * values[r + c : r + c + 1, :] for p, r in parts for c in range(6)]
    return lax.dot_general(jnp.concatenate(a, axis=0), levels, NT, preferred_element_type=F32)


def sided(groups, sides):
    plane = sides[12:13, :].astype(I32)
    level = sides[13:14, :].astype(I32)
    upper = lax.rem(lax.broadcasted_iota(I32, plane.shape, 1), 128) >= SLOTS
    x, y = plane // N, plane % N
    row = jnp.where(upper, y, y - 8)
    row = jnp.where(upper, jnp.where(y <= 5, row, -9999), jnp.where(y >= 10, row, -9999))
    levels = one_hot(jnp.where(upper, level + Z, level), 2 * Z)
    return x, row, levels


def place_own(lists, out_own, out_side):
    groups = lists.shape[0]
    first, last = own_lists(lambda g: lists[g, 16:32, :].astype(F32), groups)
    planes = one_hot(first[12:13, :].astype(I32), N * N)
    levels = one_hot(first[13:14, :].astype(I32), Z)
    first, last = first.astype(BF16), last.astype(BF16)
    for t in range(3):
        vals, row = (first, 6 * t) if t < 2 else (last, 0)
        spread = [levels * vals[row + c : row + c + 1, :] for c in range(6)]
        got = lax.dot_general(planes, jnp.concatenate(spread, axis=0), NT, preferred_element_type=F32)
        for c in range(6):
            out_own[6 * t + c] = got[:, Z * c : Z * c + Z]
    sides = lanes([lists[g, 0:16, :].astype(F32) for g in range(groups)])
    x, row, levels = sided(groups, sides)
    planes = one_hot(x * 8 + row, 8 * N)
    sides = sides.astype(BF16)
    got = place(((planes, 0), (planes, 6)), sides, levels)
    for k in range(12):
        out_side[k] = got[8 * N * k : 8 * N * k + 8 * N]


def roll_z(f, k, lane):
    moved = pltpu.roll(f, (-k) % Z, f.ndim - 1)
    keep = (lane < Z - k) if k > 0 else (lane >= -k)
    return jnp.where(keep, moved, 0.0)


def stencil(ev, es, eb, el, em):
    def total(terms):
        near = far = None
        for g, fwd in terms:
            k = 0 if fwd else -1
            p, q = g(1 + k) - g(k), g(2 + k) - g(k - 1)
            near, far = (p, q) if near is None else (near + p, far + q)
        return INNER * near + OUTER * far

    def reader(ref, x, y0, n):
        base = x * YE if isinstance(x, int) else pl.multiple_of(x * YE, 8)

        def along_x(c):
            return lambda k: ref[c, pl.ds(base + (k * YE + y0), n), :]

        def along_y(c):
            return lambda k: ref[c, pl.ds(base + (y0 + k), n), :]

        def along_z(c):
            f = ref[c, pl.ds(base + y0, n), :]
            lane = lax.broadcasted_iota(I32, (n, Z), 1)
            return lambda k: f if k == 0 else roll_z(f, k, lane)

        return along_x, along_y, along_z, pl.ds(base + y0, n)

    def velocity_at(x, y0, n):
        ax, ay, az, here = reader(es, x, y0, n)
        buoy = eb[here, :]
        forces = (
            total(((ax(0), True), (ay(3), False), (az(4), False))),
            total(((ax(3), False), (ay(1), True), (az(5), False))),
            total(((ax(4), False), (ay(5), False), (az(2), True))),
        )
        for c, f in enumerate(forces):
            ev[c, here, :] = ev[c, here, :] + buoy * f

    def stress_at(x, y0, n):
        ax, ay, az, here = reader(ev, x, y0, n)
        lam, rig = el[here, :], em[here, :]
        d1, d2, d3 = total(((ax(0), False),)), total(((ay(1), False),)), total(((az(2), False),))
        e = lam * (d1 + d2 + d3)
        two = 2.0 * rig
        rates = (
            e + two * d1,
            e + two * d2,
            e + two * d3,
            rig * total(((ay(0), True), (ax(1), True))),
            rig * total(((az(0), True), (ax(2), True))),
            rig * total(((az(1), True), (ay(2), True))),
        )
        for c, r in enumerate(rates):
            es[c, here, :] = es[c, here, :] + r

    def sweep(fn, first, last, y0, n, unroll):
        def step(x, carry):
            fn(x, y0, n)
            return carry

        lax.fori_loop(XO + first, XO + last + 1, step, 0, unroll=unroll)

    def strips(fn, sides):
        for depth, rows in sides:
            for x in (XO - depth, XO + N - 1 + depth):
                fn(x, YO + (N - rows) // 2, rows)

    return velocity_at, stress_at, sweep, strips


def at(x, y):
    return x * YE + y


def layer(msg, q, d):
    rows = msg[FACE_AT[q, d]].astype(F32)
    if d == 1:
        rows = rows + msg[LOW_AT[q]].astype(F32)
    return rows


def by_parity(odd, put, one, two):
    @pl.when(odd == 0)
    def _():
        put(two, one)

    @pl.when(odd == 1)
    def _():
        put(one, two)


def prepare(lists, ya, yb, v, s, mats, out_own, out_side, ev, es, eb, el, em):
    refs = (v, s, mats.at[0], mats.at[1], mats.at[2])
    ext = (ev, es, eb, el, em)
    for q in range(NQ):
        src, dst = part(refs, q), part(ext, q)
        for x in range(N):
            dst[at(XO + x, YO) : at(XO + x, YO) + N, :] = src[N * x : N * x + N, :]

    def put_y(low, top):
        for q in range(NQ):
            dst = part(ext, q)
            for d in range(1, DEPTH[q] + 1):
                dst[pl.ds(at(XO, YO - d), N, stride=YE), :] = layer(low, q, d)
                dst[pl.ds(at(XO, YO + N - 1 + d), N, stride=YE), :] = layer(top, q, d)

    by_parity(lax.rem(lax.axis_index("gy"), 2), put_y, ya, yb)
    place_own(lists, out_own, out_side)
    velocity_at, stress_at, sweep, _ = stencil(*ext)
    sweep(velocity_at, 2, N - 3, 8, 32, 6)
    sweep(stress_at, 4, N - 5, 8, 32, 8)


def advance(xa, xb, ca, cb, own, side, *refs):
    vout, sout, ev, es, eb, el, em, beyond, corner = refs[5:]
    odd_x = lax.rem(lax.axis_index("gx"), 2)
    ext = (ev, es, eb, el, em)

    def put_x(low, top):
        for q in range(NQ):
            dst = part(ext, q)
            for d in range(1, DEPTH[q] + 1):
                for msg, x in ((low, XO - d), (top, XO + N - 1 + d)):
                    dst[at(x, YO) : at(x, YO) + N, :] = layer(msg, q, d)

    def put_corners(low, top):
        for i, (q, d, far, m) in enumerate(CORN):
            dst = part(ext, q)
            for msg, x, back in ((low, XO - 8, 8 - m), (top, XO + N, m)):
                both = msg[i].astype(F32)
                for h in range(2):
                    rows = both[8 * h : 8 * h + 8]

                    def put(depth, rows):
                        y = YO + N - 1 + depth if h else YO - depth
                        dst[pl.ds(at(x, y), 8, stride=YE), :] = rows

                    put(d, rows)
                    if far:
                        put(far, pltpu.roll(rows, back, 0))

    by_parity(odd_x, put_x, xa, xb)
    by_parity(odd_x, put_corners, ca, cb)
    velocity_at, stress_at, sweep, strips = stencil(*ext)

    def add(c, x, y, rows):
        here = slice(at(x, y), at(x, y) + rows.shape[0])
        es[c, here, :] = es[c, here, :] + rows

    def add_own(t):
        for c in range(6):
            for x in range(N):
                add(c, XO + x, YO, own[6 * t + c, N * x : N * x + N, :])

    def add_side(t):
        for c in range(6):
            for x in range(N):
                rows = slice(8 * x, 8 * x + 8)
                add(c, XO + x, YO - 8, side[6 * t + c, rows, 0:Z])
                add(c, XO + x, YO + N, side[6 * t + c, rows, Z : 2 * Z])

    def place_beyond():
        groups = (ca.shape[0] - NCORN) * 2 // 3
        base = NCORN

        def one(msg, up, k):
            first = lanes([msg[base + groups + g].astype(F32) for g in range(groups // 2)])
            plane = first[12:13, :].astype(I32)
            levels = one_hot(first[13:14, :].astype(I32), Z)
            x, y = plane // N, plane % N

            def faces(far):
                i = x if up else x - (N - far)
                return one_hot(jnp.where(i >= 0, i * N + y, -1), far * N)

            parts = ((faces(FAR[0]), 0), (faces(FAR[1]), 6))
            beyond[k] = place(parts, first.astype(BF16), levels)
            sides = lanes([msg[base + g].astype(F32) for g in range(groups)])
            sx, row, levels = sided(groups, sides)

            def edges(near):
                i = sx if up else sx - (N - near)
                return one_hot(jnp.where(i >= 0, i * 8 + row, -1), 8 * near)

            parts = ((edges(NEAR[0]), 0), (edges(NEAR[1]), 6))
            corner[k] = place(parts, sides.astype(BF16), levels)

        @pl.when(odd_x == 0)
        def _():
            one(cb, False, 0)
            one(ca, True, 1)

        @pl.when(odd_x == 1)
        def _():
            one(ca, False, 0)
            one(cb, True, 1)

    def add_beyond(t):
        far, near = FAR[t], NEAR[t]
        f0, n0 = (0, 0) if t == 0 else (6 * N * FAR[0], 6 * 8 * NEAR[0])
        for k in range(2):
            for c in range(6):
                x0 = XO + N if k else XO - far
                for i in range(far):
                    r = f0 + N * (c * far + i)
                    add(c, x0 + i, YO, beyond[k, r : r + N, :])
                x0 = XO + N if k else XO - near
                for i in range(near):
                    r = n0 + 8 * (c * near + i)
                    add(c, x0 + i, YO - 8, corner[k, r : r + 8, 0:Z])
                    add(c, x0 + i, YO + N, corner[k, r : r + 8, Z : 2 * Z])

    place_beyond()
    sweep(velocity_at, -4, 1, 8, 32, 6)
    sweep(velocity_at, N - 2, N + 3, 8, 32, 6)
    strips(velocity_at, ((5, 24), (6, 24), (7, 16), (8, 16)))
    sweep(stress_at, -2, 3, 8, 32, 6)
    sweep(stress_at, N - 4, N + 1, 8, 32, 6)
    strips(stress_at, ((3, 24), (4, 24), (5, 24), (6, 16)))
    add_own(0)
    add_side(0)
    add_beyond(0)
    sweep(velocity_at, 0, N - 1, 8, 32, 8)
    strips(velocity_at, ((1, 24), (2, 24), (3, 24), (4, 16), (5, 16)))
    sweep(stress_at, -2, N + 1, 12, 24, 10)
    strips(stress_at, ((3, 16),))
    add_own(1)
    add_side(1)
    add_beyond(1)
    sweep(velocity_at, 0, N - 1, 12, 24, 8)
    strips(velocity_at, ((1, 16), (2, 16)))
    sweep(stress_at, 0, N - 1, 16, 16, 8)
    for x in range(N):
        here = slice(at(XO + x, YO), at(XO + x, YO) + N)
        rows = slice(N * x, N * x + N)
        for c in range(3):
            vout[c, rows, :] = ev[c, here, :]
        for c in range(6):
            sout[c, rows, :] = es[c, here, :] + own[12 + c, rows, :]


EXT = [((n, XE * YE, Z), F32) for n in (3, 6)] + [((XE * YE, Z), F32)] * 3
SCRATCH = [
    pltpu.VMEM((2, 6 * N * (FAR[0] + FAR[1]), Z), F32),
    pltpu.VMEM((2, 6 * 8 * (NEAR[0] + NEAR[1]), 2 * Z), F32),
]


def swaps(count, first):
    pairs = []
    for i in range(first, count - 1, 2):
        pairs += [(i, i + 1), (i + 1, i)]
    return pairs


def swap_both(a, b, axis):
    count = lax.axis_size(axis)
    return (
        lax.ppermute(a, axis, swaps(count, 0)),
        lax.ppermute(b, axis, swaps(count, 1)),
    )


def call(kernel, outs, args, scratch=(), flops=1_000_000, mib=8, here=True, keep=True, aliases=None):
    if not here:
        held = [pltpu.VMEM(a.shape, a.dtype) for a in args]
        args = [pltpu.with_memory_space_constraint(a, pltpu.HBM) for a in args]
        scratch = held + list(scratch) + [pltpu.SemaphoreType.DMA((len(args),))]
    return pl.pallas_call(
        kernel,
        out_shape=[(pltpu.VMEM if keep else jax.ShapeDtypeStruct)(s, t) for s, t in outs],
        in_specs=[vmem() if here else pl.BlockSpec(memory_space=pltpu.HBM)] * len(args),
        out_specs=[vmem()] * len(outs),
        scratch_shapes=list(scratch),
        input_output_aliases=aliases or {},
        compiler_params=pltpu.CompilerParams(vmem_limit_bytes=mib * 1024 * 1024),
        cost_estimate=pl.CostEstimate(flops=flops, bytes_accessed=1_000_000, transcendentals=0),
    )(*args)


def local(velocity, stresses, buoyancy, lame, rigidity, hist, mech, res, owners, cells):
    groups = lax.axis_size("gy")
    v = velocity.reshape(3, N * N, Z)
    s = stresses.reshape(6, N * N, Z)
    b, l, m = (a.reshape(N * N, Z) for a in (buoyancy, lame, rigidity))
    state = (v, s, b, l, m)
    face = ((NFACE, N, Z), BF16)
    rows = hist.shape[0]
    ya, yb, sent, mats = call(
        lambda *refs: opening(groups, *refs),
        [face, face, ((groups, 32, 128), BF16), ((3, N * N, Z), F32)],
        state + (hist, mech.T, res.T, owners.reshape(1, rows), cells.reshape(1, rows)),
        [pltpu.VMEM((32, rows), F32)],
        here=False,
    )
    later = (v, s, mats)
    ya, yb = swap_both(ya, yb, "gy")
    lists = lax.all_to_all(sent, "gy", split_axis=0, concat_axis=0, tiled=True)
    xa, xb = call(pack_x, [face, face], later)
    xa, xb = swap_both(xa, xb, "gx")
    rest = ((NCORN + groups + groups // 2, N, Z), BF16)
    ca, cb = call(pack_corners, [rest, rest], (ya, yb, lists))
    ca, cb = swap_both(ca, cb, "gx")
    own, side, *ext = call(
        prepare,
        [((18, N * N, Z), F32), ((12, 8 * N, 2 * Z), F32)] + EXT,
        (lists, ya, yb) + later,
        flops=10_000_000_000,
        mib=LIMIT[0],
    )
    vout, sout, *_ = call(
        advance,
        [(v.shape, F32), (s.shape, F32)] + EXT,
        (xa, xb, ca, cb, own, side) + tuple(ext),
        SCRATCH,
        keep=False,
        mib=LIMIT[1],
        aliases={6 + i: 2 + i for i in range(5)},
    )
    return vout.reshape(velocity.shape), sout.reshape(stresses.shape)


def solution(mesh):
    in_specs = (
        P(None, "gx", "gy", None),
        P(None, "gx", "gy", None),
        P("gx", "gy", None),
        P("gx", "gy", None),
        P("gx", "gy", None),
        P(("gx", "gy"), None),
        P(("gx", "gy"), None),
        P(),
        P(("gx", "gy"), None),
        P(("gx", "gy")),
    )
    out_specs = (P(None, "gx", "gy", None), P(None, "gx", "gy", None))
    return jax.shard_map(local, mesh=mesh, in_specs=in_specs, out_specs=out_specs, check_vma=False)
```

```python
import jax
import jax.numpy as jnp
from jax import lax
from jax.experimental import pallas as pl
from jax.experimental.pallas import tpu as pltpu
from jax.sharding import PartitionSpec as P

INNER = 9.0 / 8.0
OUTER = -1.0 / 24.0
F32, BF16, I32 = jnp.float32, jnp.bfloat16, jnp.int32

N = 16
Z = 128
XO = 11
XE = XO + N + 10
YO = 16
YE = 40
DEPTH = [9] * 6 + [8] * 3 + [8, 6, 6]
CORNER = [8] * 6 + [6] * 3 + [6, 5, 5]
NQ = len(DEPTH)
FACE = [(q, d) for q in range(NQ) for d in range(1, DEPTH[q] + 1)]
FACE_AT = {qd: i for i, qd in enumerate(FACE)}
LOW_AT = {q: len(FACE) + q for q in range(NQ)}
NFACE = len(FACE) + NQ
PACKED = {
    8: ((1, 0, 0), (2, 0, 0), (3, 7, 2), (4, 6, 3), (5, 8, 2)),
    6: ((1, 6, 2), (2, 0, 0), (3, 4, 3), (5, 0, 0)),
    5: ((1, 3, 3), (2, 4, 2), (5, 0, 0)),
}
CORN = [(q,) + unit for q in range(NQ) for unit in PACKED[CORNER[q]]]
NCORN = len(CORN)
SLOTS = 64
FLOPS = 1_000_000
LIMIT = (24, 24)
FAR = (6, 3)
NEAR = (5, 2)


def vmem():
    return pl.BlockSpec(memory_space=pltpu.VMEM)


def part(refs, q):
    v, s, b, l, m = refs
    if q < 6:
        return s.at[q]
    if q < 9:
        return v.at[q - 6]
    return (b, l, m)[q - 9]


def split(x):
    hi = x.astype(BF16)
    return hi, (x - hi.astype(F32)).astype(BF16)


def fetch(pairs, sems):
    copies = [pltpu.make_async_copy(a, b, sems.at[i]) for i, (a, b) in enumerate(pairs)]
    for copy in copies:
        copy.start()
    return copies


def opening(groups, *refs):
    given, (out_a, out_b, sent, mats), held, vals, sems = refs[:10], refs[10:14], refs[14:24], refs[24], refs[25]
    copies = fetch(list(zip(given, held)), sems)
    for copy in copies[5:]:
        copy.wait()
    route(groups, *held[5:], sent, vals)
    for copy in copies[:5]:
        copy.wait()
    pack_y(*held[:5], out_a, out_b)
    for i in range(3):
        mats[i] = held[2 + i][...]


def pack_y(v, s, b, l, m, out_a, out_b):
    odd = lax.rem(lax.axis_index("gy"), 2)
    refs = (v, s, b, l, m)
    for out, high in ((out_a, odd == 0), (out_b, odd == 1)):
        for q in range(NQ):
            src = part(refs, q)
            for d in range(1, DEPTH[q] + 1):
                y = jnp.where(high, N - d, d - 1)
                rows = src[pl.ds(y, N, stride=N), :]
                if d == 1:
                    hi, lo = split(rows)
                    out[FACE_AT[q, d]] = hi
                    out[LOW_AT[q]] = lo
                else:
                    out[FACE_AT[q, d]] = rows.astype(BF16)


def route(groups, hist, mech, res, owners, cells, out, vals):
    rows = hist.shape[0]
    nt = (((1,), (1,)), ((), ()))
    amp = lax.dot_general(res[...], hist[...], nt, preferred_element_type=F32)
    mechf = mech[...].astype(F32)
    vals[...] = jnp.zeros_like(vals)
    vals[0:6] = mechf * amp[0:1]
    vals[6:12] = mechf * amp[1:2]
    vals[16:22] = mechf * amp[2:3]
    cell = cells[...]
    vals[12:13] = (cell // Z).astype(F32)
    vals[13:14] = (cell % Z).astype(F32)
    v = vals[...].astype(BF16)
    own = owners[...]
    hits = (lax.broadcasted_iota(I32, (groups, rows), 0) == own).astype(F32)
    r0 = lax.broadcasted_iota(I32, (rows, rows), 0)
    r1 = lax.broadcasted_iota(I32, (rows, rows), 1)
    before = (r0 < r1).astype(F32).astype(BF16)
    earlier = jnp.dot(hits.astype(BF16), before, preferred_element_type=F32)
    rank = jnp.sum(hits * earlier, axis=0, keepdims=True)
    slot = own * SLOTS + rank.astype(I32)
    total = groups * SLOTS
    pick = (lax.broadcasted_iota(I32, (total, rows), 0) == slot).astype(F32).astype(BF16)
    sent = lax.dot_general(v, pick, nt, preferred_element_type=F32)
    turned = pltpu.roll(sent, SLOTS, 1)
    left = lax.broadcasted_iota(I32, (16, 2 * SLOTS), 1) < SLOTS
    zero = jnp.zeros((16, 2 * SLOTS), F32)

    def plain(j, h):
        return sent[16 * h : 16 * h + 16, 128 * j : 128 * j + 128]

    def shifted(j, h):
        j = j % (groups // 2)
        return turned[16 * h : 16 * h + 16, 128 * j : 128 * j + 128]

    for o in range(groups):
        j = o // 2
        if o % 2 == 0:
            sides = jnp.where(left, shifted(j, 0) if j else zero, plain(j, 0))
            mine = jnp.where(left, plain(j, 0), shifted(j, 1))
        else:
            last = o == groups - 1
            sides = jnp.where(left, plain(j, 0), zero if last else shifted(j + 1, 0))
            mine = jnp.where(left, shifted(j + 1, 0), plain(j, 1))
        out[o, 0:16, :] = sides.astype(BF16)
        out[o, 16:32, :] = mine.astype(BF16)


def pack_x(v, s, mats, out_a, out_b):
    odd = lax.rem(lax.axis_index("gx"), 2)
    refs = (v, s, mats.at[0], mats.at[1], mats.at[2])
    for out, high in ((out_a, odd == 0), (out_b, odd == 1)):
        for q in range(NQ):
            src = part(refs, q)
            for d in range(1, DEPTH[q] + 1):
                x = jnp.where(high, N - d, d - 1)
                rows = src[pl.ds(pl.multiple_of(x * N, N), N), :]
                if d == 1:
                    hi, lo = split(rows)
                    out[FACE_AT[q, d]] = hi
                    out[LOW_AT[q]] = lo
                else:
                    out[FACE_AT[q, d]] = rows.astype(BF16)


def pack_corners(ya, yb, lists, out_a, out_b):
    odd_x = lax.rem(lax.axis_index("gx"), 2)
    odd_y = lax.rem(lax.axis_index("gy"), 2)
    groups = lists.shape[0]
    first, _ = own_lists(lambda g: lists[g, 16:32, :].astype(F32), groups)
    first = first.astype(BF16)
    for out in (out_a, out_b):
        for g in range(groups):
            out[NCORN + g] = lists[g, 0:16, :]
        for g in range(groups // 2):
            out[NCORN + groups + g] = first[:, 128 * g : 128 * g + 128]

    def corners(low, top, out, high):
        row = lax.broadcasted_iota(I32, (8, Z), 0)
        k = 8 if high else 0
        for i, (q, d, far, m) in enumerate(CORN):
            halves = []
            for msg in (low, top):
                a = msg[FACE_AT[q, d]].astype(F32)[k : k + 8]
                if far:
                    c = msg[FACE_AT[q, far]].astype(F32)[k : k + 8]
                    if high:
                        a = jnp.where(row < m, pltpu.roll(c, m, 0), a)
                    else:
                        a = jnp.where(row >= 8 - m, pltpu.roll(c, 8 - m, 0), a)
                halves.append(a)
            out[i] = jnp.concatenate(halves, axis=0).astype(BF16)

    for px in range(2):
        for py in range(2):

            @pl.when((odd_x == px) & (odd_y == py))
            def _():
                low, top = (yb, ya) if py == 0 else (ya, yb)
                corners(low, top, out_a, px == 0)
                corners(low, top, out_b, px == 1)


def lanes(blocks):
    return jnp.concatenate(blocks, axis=1)


def own_lists(get, groups):
    left = lax.broadcasted_iota(I32, (16, 128), 1) < SLOTS
    first, last = [], []
    for i in range(groups // 2):
        a, b = get(2 * i), get(2 * i + 1)
        first.append(jnp.where(left, a, pltpu.roll(b, SLOTS, 1)))
        last.append(jnp.where(left, pltpu.roll(a, SLOTS, 1), b))
    return lanes(first), lanes(last)


def one_hot(code, count):
    width = code.shape[1]
    return (lax.broadcasted_iota(I32, (count, width), 0) == code).astype(F32).astype(BF16)


NT = (((1,), (1,)), ((), ()))


def place(parts, values, levels):
    a = [p * values[r + c : r + c + 1, :] for p, r in parts for c in range(6)]
    return lax.dot_general(jnp.concatenate(a, axis=0), levels, NT, preferred_element_type=F32)


def sided(groups, sides):
    plane = sides[12:13, :].astype(I32)
    level = sides[13:14, :].astype(I32)
    upper = lax.rem(lax.broadcasted_iota(I32, plane.shape, 1), 128) >= SLOTS
    x, y = plane // N, plane % N
    row = jnp.where(upper, y, y - 8)
    row = jnp.where(upper, jnp.where(y <= 5, row, -9999), jnp.where(y >= 10, row, -9999))
    levels = one_hot(jnp.where(upper, level + Z, level), 2 * Z)
    return x, row, levels


def place_own(lists, out_own, out_side):
    groups = lists.shape[0]
    first, last = own_lists(lambda g: lists[g, 16:32, :].astype(F32), groups)
    planes = one_hot(first[12:13, :].astype(I32), N * N)
    levels = one_hot(first[13:14, :].astype(I32), Z)
    first, last = first.astype(BF16), last.astype(BF16)
    for t in range(3):
        vals, row = (first, 6 * t) if t < 2 else (last, 0)
        spread = [levels * vals[row + c : row + c + 1, :] for c in range(6)]
        got = lax.dot_general(planes, jnp.concatenate(spread, axis=0), NT, preferred_element_type=F32)
        for c in range(6):
            out_own[6 * t + c] = got[:, Z * c : Z * c + Z]
    sides = lanes([lists[g, 0:16, :].astype(F32) for g in range(groups)])
    x, row, levels = sided(groups, sides)
    planes = one_hot(x * 8 + row, 8 * N)
    sides = sides.astype(BF16)
    got = place(((planes, 0), (planes, 6)), sides, levels)
    for k in range(12):
        out_side[k] = got[8 * N * k : 8 * N * k + 8 * N]


def roll_z(f, k, lane):
    moved = pltpu.roll(f, (-k) % Z, f.ndim - 1)
    keep = (lane < Z - k) if k > 0 else (lane >= -k)
    return jnp.where(keep, moved, 0.0)


def stencil(ev, es, eb, el, em):
    def total(terms):
        near = far = None
        for g, fwd in terms:
            k = 0 if fwd else -1
            p, q = g(1 + k) - g(k), g(2 + k) - g(k - 1)
            near, far = (p, q) if near is None else (near + p, far + q)
        return INNER * near + OUTER * far

    def reader(ref, x, y0, n):
        base = x * YE if isinstance(x, int) else pl.multiple_of(x * YE, 8)

        def along_x(c):
            return lambda k: ref[c, pl.ds(base + (k * YE + y0), n), :]

        def along_y(c):
            return lambda k: ref[c, pl.ds(base + (y0 + k), n), :]

        def along_z(c):
            f = ref[c, pl.ds(base + y0, n), :]
            lane = lax.broadcasted_iota(I32, (n, Z), 1)
            return lambda k: f if k == 0 else roll_z(f, k, lane)

        return along_x, along_y, along_z, pl.ds(base + y0, n)

    def velocity_at(x, y0, n):
        ax, ay, az, here = reader(es, x, y0, n)
        buoy = eb[here, :]
        forces = (
            total(((ax(0), True), (ay(3), False), (az(4), False))),
            total(((ax(3), False), (ay(1), True), (az(5), False))),
            total(((ax(4), False), (ay(5), False), (az(2), True))),
        )
        for c, f in enumerate(forces):
            ev[c, here, :] = ev[c, here, :] + buoy * f

    def stress_at(x, y0, n):
        ax, ay, az, here = reader(ev, x, y0, n)
        lam, rig = el[here, :], em[here, :]
        d1, d2, d3 = total(((ax(0), False),)), total(((ay(1), False),)), total(((az(2), False),))
        e = lam * (d1 + d2 + d3)
        two = 2.0 * rig
        rates = (
            e + two * d1,
            e + two * d2,
            e + two * d3,
            rig * total(((ay(0), True), (ax(1), True))),
            rig * total(((az(0), True), (ax(2), True))),
            rig * total(((az(1), True), (ay(2), True))),
        )
        for c, r in enumerate(rates):
            es[c, here, :] = es[c, here, :] + r

    def sweep(fn, first, last, y0, n, unroll):
        def step(x, carry):
            fn(x, y0, n)
            return carry

        lax.fori_loop(XO + first, XO + last + 1, step, 0, unroll=unroll)

    def strips(fn, sides):
        for depth, rows in sides:
            for x in (XO - depth, XO + N - 1 + depth):
                fn(x, YO + (N - rows) // 2, rows)

    return velocity_at, stress_at, sweep, strips


def at(x, y):
    return x * YE + y


def layer(msg, q, d):
    rows = msg[FACE_AT[q, d]].astype(F32)
    if d == 1:
        rows = rows + msg[LOW_AT[q]].astype(F32)
    return rows


def by_parity(odd, put, one, two):
    @pl.when(odd == 0)
    def _():
        put(two, one)

    @pl.when(odd == 1)
    def _():
        put(one, two)


def place_beyond(msg, up, beyond, corner, k):
    groups = (msg.shape[0] - NCORN) * 2 // 3
    first = lanes([msg[NCORN + groups + g].astype(F32) for g in range(groups // 2)])
    plane = first[12:13, :].astype(I32)
    levels = one_hot(first[13:14, :].astype(I32), Z)
    x, y = plane // N, plane % N

    def faces(far):
        i = x - jnp.where(up, 0, N - far)
        return one_hot(jnp.where(i >= 0, i * N + y, -1), far * N)

    parts = ((faces(FAR[0]), 0), (faces(FAR[1]), 6))
    beyond[k] = place(parts, first.astype(BF16), levels)
    sides = lanes([msg[NCORN + g].astype(F32) for g in range(groups)])
    sx, row, levels = sided(groups, sides)

    def edges(near):
        i = sx - jnp.where(up, 0, N - near)
        return one_hot(jnp.where(i >= 0, i * 8 + row, -1), 8 * near)

    parts = ((edges(NEAR[0]), 0), (edges(NEAR[1]), 6))
    corner[k] = place(parts, sides.astype(BF16), levels)


def prepare(lists, ya, yb, v, s, mats, out_own, out_side, ev, es, eb, el, em):
    refs = (v, s, mats.at[0], mats.at[1], mats.at[2])
    ext = (ev, es, eb, el, em)
    for q in range(NQ):
        src, dst = part(refs, q), part(ext, q)
        for x in range(N):
            dst[at(XO + x, YO) : at(XO + x, YO) + N, :] = src[N * x : N * x + N, :]

    def put_y(low, top):
        for q in range(NQ):
            dst = part(ext, q)
            for d in range(1, DEPTH[q] + 1):
                dst[pl.ds(at(XO, YO - d), N, stride=YE), :] = layer(low, q, d)
                dst[pl.ds(at(XO, YO + N - 1 + d), N, stride=YE), :] = layer(top, q, d)

    by_parity(lax.rem(lax.axis_index("gy"), 2), put_y, ya, yb)
    place_own(lists, out_own, out_side)
    velocity_at, stress_at, sweep, _ = stencil(*ext)
    sweep(velocity_at, 2, N - 3, 8, 32, 6)
    sweep(stress_at, 4, N - 5, 8, 32, 8)


def beside(ca, beyond, corner):
    place_beyond(ca, lax.rem(lax.axis_index("gx"), 2) == 0, beyond, corner, 0)


def advance(xa, xb, ca, cb, own, side, *refs):
    vout, sout, ev, es, eb, el, em, beyond, corner = refs[7:]
    odd_x = lax.rem(lax.axis_index("gx"), 2)
    ext = (ev, es, eb, el, em)

    def put_x(low, top):
        for q in range(NQ):
            dst = part(ext, q)
            for d in range(1, DEPTH[q] + 1):
                for msg, x in ((low, XO - d), (top, XO + N - 1 + d)):
                    dst[at(x, YO) : at(x, YO) + N, :] = layer(msg, q, d)

    def put_corners(low, top):
        for i, (q, d, far, m) in enumerate(CORN):
            dst = part(ext, q)
            for msg, x, back in ((low, XO - 8, 8 - m), (top, XO + N, m)):
                both = msg[i].astype(F32)
                for h in range(2):
                    rows = both[8 * h : 8 * h + 8]

                    def put(depth, rows):
                        y = YO + N - 1 + depth if h else YO - depth
                        dst[pl.ds(at(x, y), 8, stride=YE), :] = rows

                    put(d, rows)
                    if far:
                        put(far, pltpu.roll(rows, back, 0))

    by_parity(odd_x, put_x, xa, xb)
    by_parity(odd_x, put_corners, ca, cb)
    velocity_at, stress_at, sweep, strips = stencil(*ext)

    def add(c, x, y, rows):
        here = slice(at(x, y), at(x, y) + rows.shape[0])
        es[c, here, :] = es[c, here, :] + rows

    def add_own(t):
        for c in range(6):
            for x in range(N):
                add(c, XO + x, YO, own[6 * t + c, N * x : N * x + N, :])

    def add_side(t):
        for c in range(6):
            for x in range(N):
                rows = slice(8 * x, 8 * x + 8)
                add(c, XO + x, YO - 8, side[6 * t + c, rows, 0:Z])
                add(c, XO + x, YO + N, side[6 * t + c, rows, Z : 2 * Z])

    def add_beyond(t):
        far, near = FAR[t], NEAR[t]
        f0, n0 = (0, 0) if t == 0 else (6 * N * FAR[0], 6 * 8 * NEAR[0])
        for k in range(2):
            slot = jnp.where(odd_x == 1, k, 1 - k)
            for c in range(6):
                x0 = XO + N if k else XO - far
                for i in range(far):
                    r = f0 + N * (c * far + i)
                    add(c, x0 + i, YO, beyond[slot, r : r + N, :])
                x0 = XO + N if k else XO - near
                for i in range(near):
                    r = n0 + 8 * (c * near + i)
                    add(c, x0 + i, YO - 8, corner[slot, r : r + 8, 0:Z])
                    add(c, x0 + i, YO + N, corner[slot, r : r + 8, Z : 2 * Z])

    place_beyond(cb, odd_x == 1, beyond, corner, 1)
    sweep(velocity_at, -4, 1, 8, 32, 6)
    sweep(velocity_at, N - 2, N + 3, 8, 32, 6)
    strips(velocity_at, ((5, 24), (6, 24), (7, 16), (8, 16)))
    sweep(stress_at, -2, 3, 8, 32, 6)
    sweep(stress_at, N - 4, N + 1, 8, 32, 6)
    strips(stress_at, ((3, 24), (4, 24), (5, 24), (6, 16)))
    add_own(0)
    add_side(0)
    add_beyond(0)
    sweep(velocity_at, 0, N - 1, 8, 32, 8)
    strips(velocity_at, ((1, 24), (2, 24), (3, 24), (4, 16), (5, 16)))
    sweep(stress_at, -2, N + 1, 12, 24, 10)
    strips(stress_at, ((3, 16),))
    add_own(1)
    add_side(1)
    add_beyond(1)
    sweep(velocity_at, 0, N - 1, 12, 24, 8)
    strips(velocity_at, ((1, 16), (2, 16)))
    sweep(stress_at, 0, N - 1, 16, 16, 8)
    for x in range(N):
        here = slice(at(XO + x, YO), at(XO + x, YO) + N)
        rows = slice(N * x, N * x + N)
        for c in range(3):
            vout[c, rows, :] = ev[c, here, :]
        for c in range(6):
            sout[c, rows, :] = es[c, here, :] + own[12 + c, rows, :]


EXT = [((n, XE * YE, Z), F32) for n in (3, 6)] + [((XE * YE, Z), F32)] * 3
BEYOND = [
    ((2, 6 * N * (FAR[0] + FAR[1]), Z), F32),
    ((2, 6 * 8 * (NEAR[0] + NEAR[1]), 2 * Z), F32),
]


def swaps(count, first):
    pairs = []
    for i in range(first, count - 1, 2):
        pairs += [(i, i + 1), (i + 1, i)]
    return pairs


def swap_both(a, b, axis):
    count = lax.axis_size(axis)
    return (
        lax.ppermute(a, axis, swaps(count, 0)),
        lax.ppermute(b, axis, swaps(count, 1)),
    )


def call(kernel, outs, args, scratch=(), flops=1_000_000, mib=8, here=True, keep=True, aliases=None):
    if not here:
        held = [pltpu.VMEM(a.shape, a.dtype) for a in args]
        args = [pltpu.with_memory_space_constraint(a, pltpu.HBM) for a in args]
        scratch = held + list(scratch) + [pltpu.SemaphoreType.DMA((len(args),))]
    return pl.pallas_call(
        kernel,
        out_shape=[(pltpu.VMEM if keep else jax.ShapeDtypeStruct)(s, t) for s, t in outs],
        in_specs=[vmem() if here else pl.BlockSpec(memory_space=pltpu.HBM)] * len(args),
        out_specs=[vmem()] * len(outs),
        scratch_shapes=list(scratch),
        input_output_aliases=aliases or {},
        compiler_params=pltpu.CompilerParams(vmem_limit_bytes=mib * 1024 * 1024),
        cost_estimate=pl.CostEstimate(flops=flops, bytes_accessed=1_000_000, transcendentals=0),
    )(*args)


def local(velocity, stresses, buoyancy, lame, rigidity, hist, mech, res, owners, cells):
    groups = lax.axis_size("gy")
    v = velocity.reshape(3, N * N, Z)
    s = stresses.reshape(6, N * N, Z)
    b, l, m = (a.reshape(N * N, Z) for a in (buoyancy, lame, rigidity))
    state = (v, s, b, l, m)
    face = ((NFACE, N, Z), BF16)
    rows = hist.shape[0]
    ya, yb, sent, mats = call(
        lambda *refs: opening(groups, *refs),
        [face, face, ((groups, 32, 128), BF16), ((3, N * N, Z), F32)],
        state + (hist, mech.T, res.T, owners.reshape(1, rows), cells.reshape(1, rows)),
        [pltpu.VMEM((32, rows), F32)],
        here=False,
    )
    later = (v, s, mats)
    ya, yb = swap_both(ya, yb, "gy")
    lists = lax.all_to_all(sent, "gy", split_axis=0, concat_axis=0, tiled=True)
    xa, xb = call(pack_x, [face, face], later)
    xa, xb = swap_both(xa, xb, "gx")
    rest = ((NCORN + groups + groups // 2, N, Z), BF16)
    ca, cb = call(pack_corners, [rest, rest], (ya, yb, lists))
    ca, cb = swap_both(ca, cb, "gx")
    own, side, *ext = call(
        prepare,
        [((18, N * N, Z), F32), ((12, 8 * N, 2 * Z), F32)] + EXT,
        (lists, ya, yb) + later,
        flops=10_000_000_000,
        mib=LIMIT[0],
    )
    ext += call(beside, BEYOND, (ca,), flops=FLOPS, mib=16)
    vout, sout, *_ = call(
        advance,
        [(v.shape, F32), (s.shape, F32)] + EXT + BEYOND,
        (xa, xb, ca, cb, own, side) + tuple(ext),
        keep=False,
        mib=LIMIT[1],
        aliases={6 + i: 2 + i for i in range(len(EXT + BEYOND))},
    )
    return vout.reshape(velocity.shape), sout.reshape(stresses.shape)


def solution(mesh):
    in_specs = (
        P(None, "gx", "gy", None),
        P(None, "gx", "gy", None),
        P("gx", "gy", None),
        P("gx", "gy", None),
        P("gx", "gy", None),
        P(("gx", "gy"), None),
        P(("gx", "gy"), None),
        P(),
        P(("gx", "gy"), None),
        P(("gx", "gy")),
    )
    out_specs = (P(None, "gx", "gy", None), P(None, "gx", "gy", None))
    return jax.shard_map(local, mesh=mesh, in_specs=in_specs, out_specs=out_specs, check_vma=False)
```
